64 devices in a mesh: rep: 8 (over x, y, core), dp: 8 (over z).
Axes of the slice: x: 2, y: 2, z: 8, core: 2. Of those that a mesh axis runs over, the one named last changes fastest.
The devices are a block of a 4x4x8 slice.
Arguments:
- g_w_gate: bfloat16 [64, 2, 640, 1536], P(('rep', 'dp')), parts along dimension 0
- g_w_up: bfloat16 [64, 2, 640, 1536], P(('rep', 'dp')), parts along dimension 0
- g_w_down: bfloat16 [64, 2, 1536, 640], P(('rep', 'dp')), parts along dimension 0
- w_gate: bfloat16 [2, 640, 1536], replicated
- w_up: bfloat16 [2, 640, 1536], replicated
- w_down: bfloat16 [2, 1536, 640], replicated
- m_w_gate: float32 [2, 640, 1536], P(None, 'dp')
- m_w_up: float32 [2, 640, 1536], P(None, 'dp')
- m_w_down: float32 [2, 1536, 640], P(None, 'dp')
- v_w_gate: float32 [2, 640, 1536], P(None, 'dp')
- v_w_up: float32 [2, 640, 1536], P(None, 'dp')
- v_w_down: float32 [2, 1536, 640], P(None, 'dp')
Outputs:
- output 1: bfloat16 [16, 640, 1536], P('rep'), parts along dimension 0
- output 2: bfloat16 [16, 640, 1536], P('rep'), parts along dimension 0
- output 3: bfloat16 [16, 1536, 640], P('rep'), parts along dimension 0
- output 4: float32 [16, 640, 1536], P('rep', 'dp'), parts along dimension 0
- output 5: float32 [16, 640, 1536], P('rep', 'dp'), parts along dimension 0
- output 6: float32 [16, 1536, 640], P('rep', 'dp'), parts along dimension 0
- output 7: float32 [16, 640, 1536], P('rep', 'dp'), parts along dimension 0
- output 8: float32 [16, 640, 1536], P('rep', 'dp'), parts along dimension 0
- output 9: float32 [16, 1536, 640], P('rep', 'dp'), parts along dimension 0
There are 8 independent parts. The reference program is written for one: setup_inputs(seed, part) draws one part's arguments, and reference() takes and returns one part's arrays. A program takes and returns all parts, laid end to end along the dimension named above; an argument that names none is the same for every part.
All inputs are finite; a program needn't handle non-finite values.
Results may differ from the reference program's by a relative error of at most 0.022.
Values are sent between devices in bfloat16 or wider.
A program may use at most 768 MiB of HBM per device.

```python
import jax
import jax.numpy as jnp
from jax import lax

DEVICES = 8
D = 640
FF = 1536
LAYERS = 2
NAMES = ("w_gate", "w_up", "w_down")
SHAPES = {"w_gate": (LAYERS, D, FF), "w_up": (LAYERS, D, FF), "w_down": (LAYERS, FF, D)}


def setup_inputs(seed: int = 0, part: int = 0) -> dict:
    kz, *keys = jax.random.split(jax.random.key(seed), 1 + 5 * len(NAMES))
    loud = 2.0 ** jax.random.uniform(kz, (), jnp.float32, -1.0, 1.0)
    drawn = {}
    for name, key, both in zip(NAMES, keys[:3], keys[3:6], strict=True):
        own = jax.random.normal(jax.random.fold_in(key, part), (DEVICES, *SHAPES[name]), jnp.float32)
        shared = jax.random.normal(jax.random.fold_in(both, part), SHAPES[name], jnp.float32)
        drawn["g_" + name] = (loud * (0.7 * shared / DEVICES + 0.7 * own * DEVICES**-0.5)).astype(jnp.bfloat16)
    for name, key in zip(NAMES, keys[6:9], strict=True):
        drawn[name] = (jax.random.normal(key, SHAPES[name], jnp.float32) * SHAPES[name][1] ** -0.5).astype(jnp.bfloat16)
    for name, key in zip(NAMES, keys[9:12], strict=True):
        drawn["m_" + name] = loud * 0.5 * jax.random.normal(key, SHAPES[name], jnp.float32)
    for name, key in zip(NAMES, keys[12:15], strict=True):
        drawn["v_" + name] = loud * loud * jax.random.uniform(key, SHAPES[name], jnp.float32, 0.5, 1.5)
    return drawn


def adamw(w, m, v, g):
    m = 0.9 * m + 0.1 * g
    v = 0.95 * v + 0.05 * g * g
    step = m * lax.rsqrt(v + 1e-8) + 0.1 * w
    return (w - 0.02 * step).astype(jnp.bfloat16), m, v


def reference(g_w_gate, g_w_up, g_w_down, w_gate, w_up, w_down, m_w_gate, m_w_up, m_w_down, v_w_gate, v_w_up, v_w_down):
    def total(terms):
        return lax.scan(lambda so_far, term: (so_far + term.astype(jnp.float32), None), jnp.zeros(terms.shape[1:], jnp.float32), terms)[0]

    gradients = [total(terms).astype(jnp.bfloat16).astype(jnp.float32) for terms in (g_w_gate, g_w_up, g_w_down)]
    new = [
        adamw(w.astype(jnp.float32), m, v, g)
        for w, m, v, g in zip((w_gate, w_up, w_down), (m_w_gate, m_w_up, m_w_down), (v_w_gate, v_w_up, v_w_down), gradients, strict=True)
    ]
    return tuple(one[which] for which in range(3) for one in new)
```

```python
import jax
import jax.numpy as jnp
from jax import lax
from jax.experimental import pallas as pl
from jax.experimental.pallas import tpu as pltpu
from jax.sharding import PartitionSpec as P

MESH = pl.DeviceIdType.MESH
ROWS = 16


def adamw(w, m, v, g):
    m = 0.9 * m + 0.1 * g
    v = 0.95 * v + 0.05 * g * g
    step = m * lax.rsqrt(v + 1e-8) + 0.1 * w
    return (w - 0.02 * step).astype(jnp.bfloat16), m, v


def kernel(n, layers, *refs):
    refs = iter(refs)
    take = lambda k: [next(refs) for _ in range(k)]
    g_hbm, w_hbm, m_hbm, v_hbm = take(3), take(3), take(3), take(3)
    w_out, m_out, v_out = take(3), take(3), take(3)
    terms, landed = take(3), take(3)
    load_sem, own_sem, rs_send, rs_recv, ag_send, ag_recv = refs

    me = lax.axis_index("dp")
    at = lambda k: lax.rem(me + (k + 2 * n), n)
    barrier = pltpu.get_barrier_semaphore()
    chunks = [(a, layer) for layer in range(layers) for a in range(3)]
    ways = (1, -1)
    far = n // 2

    def hops(c, way):
        return far if (c % 2 == 0) == (way == 1) else n - 1 - far

    def slot(c, way, s):
        return (0 if way == 1 else hops(c, 1)) + s - 1

    def new(a, layer, k):
        rows = w_out[a].shape[1] // n
        return w_out[a].at[layer, pl.ds(pl.multiple_of(at(k) * rows, ROWS), rows)]

    loads = {}

    def load(c, k):
        a, layer = chunks[c]
        loads[c, k % n] = pltpu.make_async_copy(g_hbm[a].at[layer, at(k)], terms[a].at[layer, at(k)], load_sem.at[c * n + k % n])
        loads[c, k % n].start()

    def loaded(c, k):
        loads[c, k % n].wait()

    for s in range(far):
        for c in range(len(chunks)):
            for way in ways:
                if hops(c, way) - s > 0:
                    load(c, way * (hops(c, way) - s))
    for c in range(len(chunks)):
        load(c, 0)
    own = {}
    for c, (a, layer) in enumerate(chunks):
        own[c] = [
            pltpu.make_async_copy(w_hbm[a].at[layer, me], new(a, layer, 0), own_sem.at[3 * c]),
            pltpu.make_async_copy(m_hbm[a].at[layer], m_out[a].at[layer], own_sem.at[3 * c + 1]),
            pltpu.make_async_copy(v_hbm[a].at[layer], v_out[a].at[layer], own_sem.at[3 * c + 2]),
        ]
        for copy in own[c]:
            copy.start()

    for way in ways:
        pl.semaphore_signal(barrier, inc=1, device_id={"dp": at(way)}, device_id_type=MESH)
    pl.semaphore_wait(barrier, 2)

    def sum_copy(c, way, s):
        a, layer = chunks[c]
        left = hops(c, way) - s + 1
        source = terms[a].at[layer, at(way * left)] if s == 1 else landed[a].at[layer, slot(c, way, s - 1)]
        i = c * (n - 1) + slot(c, way, s)
        return pltpu.make_async_remote_copy(
            src_ref=source,
            dst_ref=landed[a].at[layer, slot(c, way, s)],
            send_sem=rs_send.at[i],
            recv_sem=rs_recv.at[i],
            device_id={"dp": at(way)},
            device_id_type=MESH,
        )

    def new_copy(c, way, s):
        a, layer = chunks[c]
        block = new(a, layer, -way * (s - 1))
        i = c * (n - 1) + slot(c, way, s)
        return pltpu.make_async_remote_copy(
            src_ref=block,
            dst_ref=block,
            send_sem=ag_send.at[i],
            recv_sem=ag_recv.at[i],
            device_id={"dp": at(way)},
            device_id_type=MESH,
        )

    def arrived_new(c, way, s):
        a, layer = chunks[c]
        block = new(a, layer, -way * s)
        i = c * (n - 1) + slot(c, way, s)
        pltpu.make_async_remote_copy(
            src_ref=block,
            dst_ref=block,
            send_sem=ag_send.at[i],
            recv_sem=ag_recv.at[i],
            device_id={"dp": at(way)},
            device_id_type=MESH,
        ).wait_recv()

    def each(rows, body):
        def step(i, _):
            body(pl.ds(pl.multiple_of(i * ROWS, ROWS), ROWS))
            return 0

        lax.fori_loop(0, rows // ROWS, step, 0)

    def add(c, way, s):
        a, layer = chunks[c]
        sums, mine = landed[a].at[layer, slot(c, way, s)], terms[a].at[layer, at(way * (hops(c, way) - s))]

        def body(rows):
            sums[rows] = (sums[rows].astype(jnp.float32) + mine[rows].astype(jnp.float32)).astype(jnp.bfloat16)

        each(sums.shape[0], body)

    def update(c):
        a, layer = chunks[c]
        one = landed[a].at[layer, slot(c, 1, hops(c, 1))]
        two = landed[a].at[layer, slot(c, -1, hops(c, -1))]
        mine, w, m, v = terms[a].at[layer, me], new(a, layer, 0), m_out[a].at[layer], v_out[a].at[layer]

        def body(rows):
            g = one[rows].astype(jnp.float32) + two[rows].astype(jnp.float32) + mine[rows].astype(jnp.float32)
            g = g.astype(jnp.bfloat16).astype(jnp.float32)
            w[rows], m[rows], v[rows] = adamw(w[rows].astype(jnp.float32), m[rows], v[rows], g)

        each(one.shape[0], body)

    sent = []

    def start(copy):
        copy.start()
        sent.append(copy)

    everything = [(c, way) for c in range(len(chunks)) for way in ways]
    for c, way in everything:
        loaded(c, way * hops(c, way))
        start(sum_copy(c, way, 1))
    for s in range(1, far):
        for c, way in everything:
            if s < hops(c, way):
                sum_copy(c, way, s).wait_recv()
                loaded(c, way * (hops(c, way) - s))
                add(c, way, s)
                start(sum_copy(c, way, s + 1))
    for c in range(len(chunks)):
        for copy in own[c]:
            copy.wait()
        loaded(c, 0)
        for way in ways:
            sum_copy(c, way, hops(c, way)).wait_recv()
        update(c)
        for way in ways:
            start(new_copy(c, way, 1))
    for s in range(1, far + 1):
        for c, way in everything:
            if s <= hops(c, way):
                arrived_new(c, way, s)
                if s < hops(c, way):
                    start(new_copy(c, way, s + 1))
    for copy in sent:
        copy.wait_send()


def solution(mesh):
    n = mesh.shape["dp"]

    def step(*arrays):
        terms, weights, m, v = (arrays[i : i + 3] for i in (0, 3, 6, 9))
        layers = weights[0].shape[0]
        blocked = lambda w: w.reshape(layers, n, w.shape[-2] // n, w.shape[-1])
        whole = [jax.ShapeDtypeStruct(w.shape, w.dtype) for w in weights]
        terms, weights = [blocked(t[0]) for t in terms], [blocked(w) for w in weights]
        like = lambda x: pltpu.VMEM(x.shape, x.dtype)
        arrivals = layers * 3 * (n - 1)
        return pl.pallas_call(
            lambda *refs: kernel(n, layers, *refs),
            name="step",
            out_shape=[like(x) for x in (*whole, *m, *v)],
            in_specs=[pl.BlockSpec(memory_space=pltpu.HBM)] * 12,
            out_specs=[pl.BlockSpec(memory_space=pltpu.VMEM)] * 9,
            scratch_shapes=[
                *(pltpu.VMEM(w.shape, w.dtype) for w in weights),
                *(pltpu.VMEM((layers, n - 1, *w.shape[2:]), w.dtype) for w in weights),
                pltpu.SemaphoreType.DMA((layers * 3 * n,)),
                pltpu.SemaphoreType.DMA((layers * 3 * 3,)),
                *(pltpu.SemaphoreType.DMA((arrivals,)) for _ in range(4)),
            ],
            compiler_params=pltpu.CompilerParams(collective_id=0, has_side_effects=True, vmem_limit_bytes=40 << 20),
        )(*(pltpu.with_memory_space_constraint(x, pltpu.HBM) for x in (*terms, *weights, *m, *v)))

    all_of, cut = P(None, None, None), P(None, "dp", None)
    return jax.shard_map(
        step,
        mesh=mesh,
        in_specs=(P(("rep", "dp"), None, None, None),) * 3 + (all_of,) * 3 + (cut,) * 6,
        out_specs=(P("rep", None, None),) * 3 + (P("rep", "dp", None),) * 6,
        check_vma=False,
    )
```

```python
import jax
import jax.numpy as jnp
from jax import lax
from jax.experimental import pallas as pl
from jax.experimental.pallas import tpu as pltpu
from jax.sharding import PartitionSpec as P

MESH = pl.DeviceIdType.MESH
ROWS = 16


def adamw(w, m, v, g):
    m = 0.9 * m + 0.1 * g
    v = 0.95 * v + 0.05 * g * g
    step = m * lax.rsqrt(v + 1e-8) + 0.1 * w
    return (w - 0.02 * step).astype(jnp.bfloat16), m, v


def kernel(n, layers, *refs):
    refs = iter(refs)
    take = lambda k: [next(refs) for _ in range(k)]
    g_hbm, w_hbm, m_hbm, v_hbm = take(3), take(3), take(3), take(3)
    w_out, m_out, v_out = take(3), take(3), take(3)
    terms, landed = take(3), take(3)
    load_sem, own_sem, rs_send, rs_recv, ag_send, ag_recv = refs

    me = lax.axis_index("dp")
    at = lambda k: lax.rem(me + (k + 2 * n), n)
    barrier = pltpu.get_barrier_semaphore()
    chunks = [(a, layer) for layer in range(layers) for a in range(3)]
    ways = (1, -1)
    far = n // 2

    def hops(c, way):
        return far if (c % 2 == 0) == (way == 1) else n - 1 - far

    def slot(c, way, s):
        return (0 if way == 1 else hops(c, 1)) + s - 1

    def new(a, layer, k):
        rows = w_out[a].shape[1] // n
        return w_out[a].at[layer, pl.ds(pl.multiple_of(at(k) * rows, ROWS), rows)]

    loads = {}

    def load(c, k):
        a, layer = chunks[c]
        loads[c, k % n] = pltpu.make_async_copy(g_hbm[a].at[layer, at(k)], terms[a].at[layer, at(k)], load_sem.at[c * n + k % n])
        loads[c, k % n].start()

    def loaded(c, k):
        loads[c, k % n].wait()

    for s in range(far):
        for c in range(len(chunks)):
            for way in ways:
                if hops(c, way) - s > 0:
                    load(c, way * (hops(c, way) - s))
    for c in range(len(chunks)):
        load(c, 0)
    own = {}
    for c, (a, layer) in enumerate(chunks):
        own[c] = [
            pltpu.make_async_copy(w_hbm[a].at[layer, me], new(a, layer, 0), own_sem.at[3 * c]),
            pltpu.make_async_copy(m_hbm[a].at[layer], m_out[a].at[layer], own_sem.at[3 * c + 1]),
            pltpu.make_async_copy(v_hbm[a].at[layer], v_out[a].at[layer], own_sem.at[3 * c + 2]),
        ]
        for copy in own[c]:
            copy.start()

    for way in ways:
        pl.semaphore_signal(barrier, inc=1, device_id={"dp": at(way)}, device_id_type=MESH)
    pl.semaphore_wait(barrier, 2)

    def sum_copy(c, way, s):
        a, layer = chunks[c]
        left = hops(c, way) - s + 1
        source = terms[a].at[layer, at(way * left)] if s == 1 else landed[a].at[layer, slot(c, way, s - 1)]
        i = c * (n - 1) + slot(c, way, s)
        return pltpu.make_async_remote_copy(
            src_ref=source,
            dst_ref=landed[a].at[layer, slot(c, way, s)],
            send_sem=rs_send.at[i],
            recv_sem=rs_recv.at[i],
            device_id={"dp": at(way)},
            device_id_type=MESH,
        )

    def new_copy(c, way, s):
        a, layer = chunks[c]
        block = new(a, layer, -way * (s - 1))
        i = c * (n - 1) + slot(c, way, s)
        return pltpu.make_async_remote_copy(
            src_ref=block,
            dst_ref=block,
            send_sem=ag_send.at[i],
            recv_sem=ag_recv.at[i],
            device_id={"dp": at(way)},
            device_id_type=MESH,
        )

    def arrived_new(c, way, s):
        a, layer = chunks[c]
        block = new(a, layer, -way * s)
        i = c * (n - 1) + slot(c, way, s)
        pltpu.make_async_remote_copy(
            src_ref=block,
            dst_ref=block,
            send_sem=ag_send.at[i],
            recv_sem=ag_recv.at[i],
            device_id={"dp": at(way)},
            device_id_type=MESH,
        ).wait_recv()

    def each(rows, body):
        def step(i, _):
            body(pl.ds(pl.multiple_of(i * ROWS, ROWS), ROWS))
            return 0

        lax.fori_loop(0, rows // ROWS, step, 0)

    def add(c, way, s):
        a, layer = chunks[c]
        sums, mine = landed[a].at[layer, slot(c, way, s)], terms[a].at[layer, at(way * (hops(c, way) - s))]

        def body(rows):
            sums[rows] = (sums[rows].astype(jnp.float32) + mine[rows].astype(jnp.float32)).astype(jnp.bfloat16)

        each(sums.shape[0], body)

    def update(c):
        a, layer = chunks[c]
        one = landed[a].at[layer, slot(c, 1, hops(c, 1))]
        two = landed[a].at[layer, slot(c, -1, hops(c, -1))]
        mine, w, m, v = terms[a].at[layer, me], new(a, layer, 0), m_out[a].at[layer], v_out[a].at[layer]

        def body(rows):
            g = one[rows].astype(jnp.float32) + two[rows].astype(jnp.float32) + mine[rows].astype(jnp.float32)
            g = g.astype(jnp.bfloat16).astype(jnp.float32)
            w[rows], m[rows], v[rows] = adamw(w[rows].astype(jnp.float32), m[rows], v[rows], g)

        each(one.shape[0], body)

    sent = []

    def start(copy):
        copy.start()
        sent.append(copy)

    everything = [(c, way) for c in range(len(chunks)) for way in ways]
    for c, way in everything:
        loaded(c, way * hops(c, way))
        start(sum_copy(c, way, 1))
    for s in range(1, far):
        for c, way in everything:
            if s < hops(c, way):
                sum_copy(c, way, s).wait_recv()
                loaded(c, way * (hops(c, way) - s))
                add(c, way, s)
                start(sum_copy(c, way, s + 1))
    for c in range(len(chunks)):
        for copy in own[c]:
            copy.wait()
        loaded(c, 0)
        for way in ways:
            sum_copy(c, way, hops(c, way)).wait_recv()
        update(c)
        for way in ways:
            start(new_copy(c, way, 1))
    for s in range(1, far + 1):
        for c, way in everything:
            if s <= hops(c, way):
                arrived_new(c, way, s)
                if s < hops(c, way):
                    start(new_copy(c, way, s + 1))
    for copy in sent:
        copy.wait_send()


def put(*refs):
    *refs, sem = refs
    k = len(refs) // 2
    copies = [pltpu.make_async_copy(a, b, sem.at[i]) for i, (a, b) in enumerate(zip(refs[:k], refs[k:], strict=True))]
    for copy in copies:
        copy.start()
    for copy in copies:
        copy.wait()


def solution(mesh):
    n = mesh.shape["dp"]

    def step(*arrays):
        terms, weights, m, v = (arrays[i : i + 3] for i in (0, 3, 6, 9))
        layers = weights[0].shape[0]
        blocked = lambda w: w.reshape(layers, n, w.shape[-2] // n, w.shape[-1])
        whole = [jax.ShapeDtypeStruct(w.shape, w.dtype) for w in weights]
        terms, weights = [blocked(t[0]) for t in terms], [blocked(w) for w in weights]
        like = lambda x: pltpu.VMEM(x.shape, x.dtype)
        arrivals = layers * 3 * (n - 1)
        out = pl.pallas_call(
            lambda *refs: kernel(n, layers, *refs),
            name="step",
            out_shape=[like(x) for x in (*whole, *m, *v)],
            in_specs=[pl.BlockSpec(memory_space=pltpu.HBM)] * 12,
            out_specs=[pl.BlockSpec(memory_space=pltpu.VMEM)] * 9,
            scratch_shapes=[
                *(pltpu.VMEM(w.shape, w.dtype) for w in weights),
                *(pltpu.VMEM((layers, n - 1, *w.shape[2:]), w.dtype) for w in weights),
                pltpu.SemaphoreType.DMA((layers * 3 * n,)),
                pltpu.SemaphoreType.DMA((layers * 3 * 3,)),
                *(pltpu.SemaphoreType.DMA((arrivals,)) for _ in range(4)),
            ],
            compiler_params=pltpu.CompilerParams(collective_id=0, has_side_effects=True, vmem_limit_bytes=40 << 20),
        )(*(pltpu.with_memory_space_constraint(x, pltpu.HBM) for x in (*terms, *weights, *m, *v)))
        return pl.pallas_call(
            put,
            name="put",
            out_shape=[jax.ShapeDtypeStruct(x.shape, x.dtype) for x in out],
            in_specs=[pl.BlockSpec(memory_space=pltpu.VMEM)] * 9,
            out_specs=[pl.BlockSpec(memory_space=pl.ANY)] * 9,
            scratch_shapes=[pltpu.SemaphoreType.DMA((9,))],
            compiler_params=pltpu.CompilerParams(has_side_effects=True, vmem_limit_bytes=20 << 20),
        )(*(pltpu.with_memory_space_constraint(x, pltpu.VMEM) for x in out))

    all_of, cut = P(None, None, None), P(None, "dp", None)
    return jax.shard_map(
        step,
        mesh=mesh,
        in_specs=(P(("rep", "dp"), None, None, None),) * 3 + (all_of,) * 3 + (cut,) * 6,
        out_specs=(P("rep", None, None),) * 3 + (P("rep", "dp", None),) * 6,
        check_vma=False,
    )
```

```python
import jax
import jax.numpy as jnp
from jax import lax
from jax.experimental import pallas as pl
from jax.experimental.pallas import tpu as pltpu
from jax.sharding import PartitionSpec as P

MESH = pl.DeviceIdType.MESH
ROWS = 16
LATE = 1
WAYS = (1, -1)


def adamw(w, m, v, g):
    m = 0.9 * m + 0.1 * g
    v = 0.95 * v + 0.05 * g * g
    step = m * lax.rsqrt(v + 1e-8) + 0.1 * w
    return (w - 0.02 * step).astype(jnp.bfloat16), m, v


class Ring:
    def __init__(self, n, layers):
        self.n, self.layers, self.far = n, layers, n // 2
        self.chunks = [(a, layer) for layer in range(layers) for a in range(3)]
        self.both = [(c, way) for c in range(len(self.chunks)) for way in WAYS]
        self.arrivals = len(self.chunks) * (n - 1)

    def at(self, k):
        return lax.rem(lax.axis_index("dp") + (k + 2 * self.n), self.n)

    def waits(self):
        return lax.rem(lax.axis_index("rep"), 2) == 1

    def hops(self, c, way):
        return self.far if (c % 2 == 0) == (way == 1) else self.n - 1 - self.far

    def slot(self, c, way, s):
        return (0 if way == 1 else self.hops(c, 1)) + s - 1

    def late(self, c, s):
        return s >= self.far - (c >= len(self.chunks) - LATE)

    def late_hops(self):
        return [(c, way, s) for c, way in self.both for s in range(1, self.hops(c, way) + 1) if self.late(c, s)]

    def new(self, ref, layer, k):
        rows = ref.shape[1] // self.n
        return ref.at[layer, pl.ds(pl.multiple_of(self.at(k) * rows, ROWS), rows)]

    def greet(self):
        barrier = pltpu.get_barrier_semaphore()
        for way in WAYS:
            pl.semaphore_signal(barrier, inc=1, device_id={"dp": self.at(way)}, device_id_type=MESH)
        pl.semaphore_wait(barrier, 2)

    def send(self, source, target, send_sem, recv_sem, way):
        return pltpu.make_async_remote_copy(
            src_ref=source, dst_ref=target, send_sem=send_sem, recv_sem=recv_sem, device_id={"dp": self.at(way)}, device_id_type=MESH
        )


def each(rows, body):
    def step(i, _):
        body(pl.ds(pl.multiple_of(i * ROWS, ROWS), ROWS))
        return 0

    lax.fori_loop(0, rows // ROWS, step, 0)


def kernel(ring, *refs):
    refs = iter(refs)
    take = lambda k: [next(refs) for _ in range(k)]
    g_hbm, w_hbm, m_hbm, v_hbm = take(3), take(3), take(3), take(3)
    w_out, m_out, v_out = take(3), take(3), take(3)
    terms, landed = take(3), take(3)
    load_sem, own_sem, rs_send, rs_recv, ag_send, ag_recv = refs
    n, far, chunks, at, hops, slot = ring.n, ring.far, ring.chunks, ring.at, ring.hops, ring.slot

    loads = {}

    def load(c, k):
        a, layer = chunks[c]
        loads[c, k % n] = pltpu.make_async_copy(g_hbm[a].at[layer, at(k)], terms[a].at[layer, at(k)], load_sem.at[c * n + k % n])
        loads[c, k % n].start()

    def loaded(c, k):
        loads[c, k % n].wait()

    for s in range(far):
        for c, way in ring.both:
            if hops(c, way) - s > 0:
                load(c, way * (hops(c, way) - s))
    for c in range(len(chunks)):
        load(c, 0)
    own = {}
    for c, (a, layer) in enumerate(chunks):
        own[c] = [
            pltpu.make_async_copy(w_hbm[a].at[layer, at(0)], ring.new(w_out[a], layer, 0), own_sem.at[3 * c]),
            pltpu.make_async_copy(m_hbm[a].at[layer], m_out[a].at[layer], own_sem.at[3 * c + 1]),
            pltpu.make_async_copy(v_hbm[a].at[layer], v_out[a].at[layer], own_sem.at[3 * c + 2]),
        ]
        for copy in own[c]:
            copy.start()

    ring.greet()

    def sum_copy(c, way, s):
        a, layer = chunks[c]
        left = hops(c, way) - s + 1
        source = terms[a].at[layer, at(way * left)] if s == 1 else landed[a].at[layer, slot(c, way, s - 1)]
        i = c * (n - 1) + slot(c, way, s)
        return ring.send(source, landed[a].at[layer, slot(c, way, s)], rs_send.at[i], rs_recv.at[i], way)

    def new_copy(c, way, s, k):
        a, layer = chunks[c]
        block = ring.new(w_out[a], layer, k)
        i = c * (n - 1) + slot(c, way, s)
        return ring.send(block, block, ag_send.at[i], ag_recv.at[i], way)

    def add(c, way, s):
        a, layer = chunks[c]
        sums, mine = landed[a].at[layer, slot(c, way, s)], terms[a].at[layer, at(way * (hops(c, way) - s))]

        def body(rows):
            sums[rows] = (sums[rows].astype(jnp.float32) + mine[rows].astype(jnp.float32)).astype(jnp.bfloat16)

        each(sums.shape[0], body)

    def update(c):
        a, layer = chunks[c]
        one = landed[a].at[layer, slot(c, 1, hops(c, 1))]
        two = landed[a].at[layer, slot(c, -1, hops(c, -1))]
        mine, w, m, v = terms[a].at[layer, at(0)], ring.new(w_out[a], layer, 0), m_out[a].at[layer], v_out[a].at[layer]

        def body(rows):
            g = one[rows].astype(jnp.float32) + two[rows].astype(jnp.float32) + mine[rows].astype(jnp.float32)
            g = g.astype(jnp.bfloat16).astype(jnp.float32)
            w[rows], m[rows], v[rows] = adamw(w[rows].astype(jnp.float32), m[rows], v[rows], g)

        each(one.shape[0], body)

    sent = []

    def start(copy):
        copy.start()
        sent.append(copy)

    for c, way in ring.both:
        loaded(c, way * hops(c, way))
        start(sum_copy(c, way, 1))
    for s in range(1, far):
        for c, way in ring.both:
            if s < hops(c, way):
                sum_copy(c, way, s).wait_recv()
                loaded(c, way * (hops(c, way) - s))
                add(c, way, s)
                start(sum_copy(c, way, s + 1))
    for c in range(len(chunks)):
        for copy in own[c]:
            copy.wait()
        loaded(c, 0)
        for way in WAYS:
            sum_copy(c, way, hops(c, way)).wait_recv()
        update(c)
        for way in WAYS:
            start(new_copy(c, way, 1, 0))

    def unless_late(late, body):
        if late:
            pl.when(jnp.logical_not(ring.waits()))(body)
        else:
            body()

    for s in range(1, far + 1):
        for c, way in ring.both:
            if s <= hops(c, way):
                unless_late(ring.late(c, s), new_copy(c, way, s, -way * s).wait_recv)
                if s < hops(c, way):
                    unless_late(ring.late(c, s + 1), new_copy(c, way, s + 1, -way * s).start)
    for copy in sent:
        copy.wait_send()
    for c, way in ring.both:
        for s in range(2, hops(c, way) + 1):
            unless_late(ring.late(c, s), new_copy(c, way, s, -way * (s - 1)).wait_send)


def place(ring, c, way, s):
    a, layer = ring.chunks[c]
    return (a, layer, 0) if s == ring.far else (a, layer, 1 if way == 1 else 2)


def last(ring, *refs):
    w, out = refs[:3], refs[3:6]
    send_sem, recv_sem = refs[6:]
    late = ring.late_hops()
    ring.greet()

    def copy(c, way, s):
        a, layer = ring.chunks[c]
        if ring.late(c, s - 1):
            b, *where = place(ring, c, way, s - 1)
            source = out[b].at[*where]
        else:
            source = ring.new(w[a], layer, -way * (s - 1))
        b, *where = place(ring, c, way, s)
        i = late.index((c, way, s))
        return ring.send(source, out[b].at[*where], send_sem.at[i], recv_sem.at[i], way)

    @pl.when(ring.waits())
    def _():
        first = [hop for hop in late if not ring.late(hop[0], hop[2] - 1)]
        then = [hop for hop in late if hop not in first]
        for hop in sorted(first, key=lambda hop: hop[2]):
            copy(*hop).start()
        for c, way, s in then:
            copy(c, way, s - 1).wait_recv()
            copy(c, way, s).start()
        for c, way, s in late:
            if not ((c, way, s + 1) in late):
                copy(c, way, s).wait_recv()
        for hop in late:
            copy(*hop).wait_send()


def put(*refs):
    *refs, sem = refs
    k = len(refs) // 2
    copies = [pltpu.make_async_copy(a, b, sem.at[i]) for i, (a, b) in enumerate(zip(refs[:k], refs[k:], strict=True))]
    for copy in copies:
        copy.start()
    for copy in copies:
        copy.wait()


def put_last(ring, *refs):
    blocks, _, whole, sem = refs[:3], refs[3:6], refs[6:9], refs[9]

    @pl.when(ring.waits())
    def _():
        copies = []
        for i, (c, way, s) in enumerate(ring.late_hops()):
            a, layer, which = place(ring, c, way, s)
            copies.append(pltpu.make_async_copy(blocks[a].at[layer, which], ring.new(whole[a], layer, -way * s), sem.at[i]))
        for copy in copies:
            copy.start()
        for copy in copies:
            copy.wait()


def solution(mesh):
    n = mesh.shape["dp"]

    def step(*arrays):
        terms, weights, m, v = (arrays[i : i + 3] for i in (0, 3, 6, 9))
        ring = Ring(n, weights[0].shape[0])
        blocked = lambda w: w.reshape(ring.layers, n, w.shape[-2] // n, w.shape[-1])
        vmem = lambda x: pltpu.VMEM(x.shape, x.dtype)
        hbm = lambda x: pltpu.HBM(x.shape, x.dtype)
        keep = lambda space, arrays: [pltpu.with_memory_space_constraint(x, space) for x in arrays]
        spec = lambda space, k: [pl.BlockSpec(memory_space=space)] * k
        blocks = [blocked(w) for w in weights]
        arrived = [jax.ShapeDtypeStruct((ring.layers, n - 1, *b.shape[2:]), b.dtype) for b in blocks]
        ends = [jax.ShapeDtypeStruct((ring.layers, 3, *b.shape[2:]), b.dtype) for b in blocks]
        late = len(ring.late_hops())

        out = pl.pallas_call(
            lambda *refs: kernel(ring, *refs),
            name="step",
            out_shape=[vmem(x) for x in (*weights, *m, *v)],
            in_specs=spec(pltpu.HBM, 12),
            out_specs=spec(pltpu.VMEM, 9),
            scratch_shapes=[
                *(pltpu.VMEM(x.shape, x.dtype) for x in (*blocks, *arrived)),
                pltpu.SemaphoreType.DMA((len(ring.chunks) * n,)),
                pltpu.SemaphoreType.DMA((len(ring.chunks) * 3,)),
                *(pltpu.SemaphoreType.DMA((ring.arrivals,)) for _ in range(4)),
            ],
            compiler_params=pltpu.CompilerParams(collective_id=0, has_side_effects=True, vmem_limit_bytes=40 << 20),
        )(*keep(pltpu.HBM, [blocked(t[0]) for t in terms] + blocks + [*m, *v]))
        stored = pl.pallas_call(
            put,
            name="put",
            out_shape=[hbm(x) for x in out],
            in_specs=spec(pltpu.VMEM, 9),
            out_specs=spec(pltpu.HBM, 9),
            scratch_shapes=[pltpu.SemaphoreType.DMA((9,))],
            compiler_params=pltpu.CompilerParams(has_side_effects=True, vmem_limit_bytes=20 << 20),
        )(*keep(pltpu.VMEM, out))
        rest = pl.pallas_call(
            lambda *refs: last(ring, *refs),
            name="last",
            out_shape=[vmem(x) for x in ends],
            in_specs=spec(pltpu.VMEM, 3),
            out_specs=spec(pltpu.VMEM, 3),
            scratch_shapes=[pltpu.SemaphoreType.DMA((late,)), pltpu.SemaphoreType.DMA((late,))],
            compiler_params=pltpu.CompilerParams(collective_id=1, has_side_effects=True, vmem_limit_bytes=20 << 20),
        )(*keep(pltpu.VMEM, out[:3]))
        whole = pl.pallas_call(
            lambda *refs: put_last(ring, *refs),
            name="put_last",
            out_shape=[hbm(w) for w in weights],
            in_specs=spec(pltpu.VMEM, 3) + spec(pltpu.HBM, 3),
            out_specs=spec(pltpu.HBM, 3),
            input_output_aliases={3: 0, 4: 1, 5: 2},
            scratch_shapes=[pltpu.SemaphoreType.DMA((late,))],
            compiler_params=pltpu.CompilerParams(has_side_effects=True, vmem_limit_bytes=20 << 20),
        )(*keep(pltpu.VMEM, rest), *keep(pltpu.HBM, stored[:3]))
        return (*whole, *stored[3:])

    all_of, cut = P(None, None, None), P(None, "dp", None)
    return jax.shard_map(
        step,
        mesh=mesh,
        in_specs=(P(("rep", "dp"), None, None, None),) * 3 + (all_of,) * 3 + (cut,) * 6,
        out_specs=(P("rep", None, None),) * 3 + (P("rep", "dp", None),) * 6,
        check_vma=False,
    )
```

```python
import jax
import jax.numpy as jnp
from jax import lax
from jax.experimental import pallas as pl
from jax.experimental.pallas import tpu as pltpu
from jax.sharding import PartitionSpec as P

MESH = pl.DeviceIdType.MESH
ROWS = 16
LATE = 2
WAYS = (1, -1)


def adamw(w, m, v, g):
    m = 0.9 * m + 0.1 * g
    v = 0.95 * v + 0.05 * g * g
    step = m * lax.rsqrt(v + 1e-8) + 0.1 * w
    return (w - 0.02 * step).astype(jnp.bfloat16), m, v


class Ring:
    def __init__(self, n, layers):
        self.n, self.layers, self.far = n, layers, n // 2
        self.chunks = [(a, layer) for layer in range(layers) for a in range(3)]
        self.both = [(c, way) for c in range(len(self.chunks)) for way in WAYS]
        self.arrivals = len(self.chunks) * (n - 1)

    def at(self, k):
        return lax.rem(lax.axis_index("dp") + (k + 2 * self.n), self.n)

    def waits(self):
        return lax.rem(lax.axis_index("rep"), 2) == 0

    def hops(self, c, way):
        return self.far if (c % 2 == 0) == (way == 1) else self.n - 1 - self.far

    def slot(self, c, way, s):
        return (0 if way == 1 else self.hops(c, 1)) + s - 1

    def late(self, c, s):
        return s >= self.far - (c >= len(self.chunks) - LATE)

    def late_hops(self):
        return [(c, way, s) for c, way in self.both for s in range(1, self.hops(c, way) + 1) if self.late(c, s)]

    def span(self, ref, count):
        rows = ref.shape[1] // self.n
        if count <= self.n:
            return ref.at[0, pl.ds(0, count * rows)]
        assert count % 2 == 0 and count <= 2 * self.n
        return ref.at[pl.ds(0, 2), pl.ds(0, count // 2 * rows)]

    def done(self, ref, count, sem):
        part = self.span(ref, count)
        pltpu.make_async_copy(part, part, sem).wait()

    def new(self, ref, layer, k):
        rows = ref.shape[1] // self.n
        return ref.at[layer, pl.ds(pl.multiple_of(self.at(k) * rows, ROWS), rows)]

    def greet(self):
        for way in WAYS:
            pl.semaphore_signal(pltpu.get_barrier_semaphore(), inc=1, device_id={"dp": self.at(way)}, device_id_type=MESH)

    def greeted(self):
        pl.semaphore_wait(pltpu.get_barrier_semaphore(), 2)

    def send(self, source, target, send_sem, recv_sem, way):
        return pltpu.make_async_remote_copy(
            src_ref=source, dst_ref=target, send_sem=send_sem, recv_sem=recv_sem, device_id={"dp": self.at(way)}, device_id_type=MESH
        )


def each(rows, body):
    def step(i, _):
        body(pl.ds(pl.multiple_of(i * ROWS, ROWS), ROWS))
        return 0

    lax.fori_loop(0, rows // ROWS, step, 0)


def kernel(ring, *refs):
    refs = iter(refs)
    take = lambda k: [next(refs) for _ in range(k)]
    g_hbm, w_hbm, m_hbm, v_hbm = take(3), take(3), take(3), take(3)
    w_out, m_out, v_out = take(3), take(3), take(3)
    terms, landed = take(3), take(3)
    first_sem, load_sem, own_sem, rs_send, rs_recv, ag_send, ag_recv = refs
    n, far, chunks, at, hops, slot = ring.n, ring.far, ring.chunks, ring.at, ring.hops, ring.slot

    def load(c, k, sem):
        a, layer = chunks[c]
        return pltpu.make_async_copy(g_hbm[a].at[layer, at(k)], terms[a].at[layer, at(k)], sem)

    def first(i):
        c, way = ring.both[i]
        return load(c, way * hops(c, way), first_sem.at[i])

    def others(c):
        return [k for k in range(n) if k not in [way * hops(c, way) % n for way in WAYS]]

    def loaded(c):
        a, layer = chunks[c]
        some = pl.ds(0, len(others(c)))
        pltpu.make_async_copy(g_hbm[a].at[layer, some], terms[a].at[layer, some], load_sem.at[c]).wait()

    ring.greet()
    for i in range(len(ring.both)):
        first(i).start()

    def sum_copy(c, way, s):
        a, layer = chunks[c]
        left = hops(c, way) - s + 1
        source = terms[a].at[layer, at(way * left)] if s == 1 else landed[a].at[layer, slot(c, way, s - 1)]
        i = c * (n - 1) + slot(c, way, s)
        return ring.send(source, landed[a].at[layer, slot(c, way, s)], rs_send.at[a], rs_recv.at[i], way)

    def new_copy(c, way, s, k):
        a, layer = chunks[c]
        block = ring.new(w_out[a], layer, k)
        i = c * (n - 1) + slot(c, way, s)
        return ring.send(block, block, ag_send.at[2 * c + ring.late(c, s)], ag_recv.at[i], way)

    def add(c, way, s):
        a, layer = chunks[c]
        sums, mine = landed[a].at[layer, slot(c, way, s)], terms[a].at[layer, at(way * (hops(c, way) - s))]

        def body(rows):
            sums[rows] = (sums[rows].astype(jnp.float32) + mine[rows].astype(jnp.float32)).astype(jnp.bfloat16)

        each(sums.shape[0], body)

    def update(c):
        a, layer = chunks[c]
        one = landed[a].at[layer, slot(c, 1, hops(c, 1))]
        two = landed[a].at[layer, slot(c, -1, hops(c, -1))]
        mine, w, m, v = terms[a].at[layer, at(0)], ring.new(w_out[a], layer, 0), m_out[a].at[layer], v_out[a].at[layer]

        def body(rows):
            g = one[rows].astype(jnp.float32) + two[rows].astype(jnp.float32) + mine[rows].astype(jnp.float32)
            g = g.astype(jnp.bfloat16).astype(jnp.float32)
            w[rows], m[rows], v[rows] = adamw(w[rows].astype(jnp.float32), m[rows], v[rows], g)

        each(one.shape[0], body)

    ring.greeted()
    for i, (c, way) in enumerate(ring.both):
        first(i).wait()
        sum_copy(c, way, 1).start()
    for c, (a, layer) in enumerate(chunks):
        for k in others(c):
            load(c, k, load_sem.at[c]).start()
    for c, (a, layer) in enumerate(chunks):
        pltpu.make_async_copy(w_hbm[a].at[layer, at(0)], ring.new(w_out[a], layer, 0), own_sem.at[0]).start()
    for a in range(3):
        pltpu.make_async_copy(m_hbm[a], m_out[a], own_sem.at[1 + a]).start()
        pltpu.make_async_copy(v_hbm[a], v_out[a], own_sem.at[4 + a]).start()

    for s in range(1, far):
        for c, way in ring.both:
            if s == 1 and way == WAYS[0]:
                loaded(c)
            if s < hops(c, way):
                sum_copy(c, way, s).wait_recv()
                add(c, way, s)
                sum_copy(c, way, s + 1).start()
    ring.done(w_out[0], len(chunks), own_sem.at[0])
    for a in range(3):
        pltpu.make_async_copy(m_hbm[a], m_out[a], own_sem.at[1 + a]).wait()
        pltpu.make_async_copy(v_hbm[a], v_out[a], own_sem.at[4 + a]).wait()
    for c in range(len(chunks)):
        for way in WAYS:
            sum_copy(c, way, hops(c, way)).wait_recv()
        update(c)
        for way in WAYS:
            new_copy(c, way, 1, 0).start()

    def unless_late(late, body):
        if late:
            pl.when(jnp.logical_not(ring.waits()))(body)
        else:
            body()

    for s in range(1, far + 1):
        for c, way in ring.both:
            if s <= hops(c, way):
                unless_late(ring.late(c, s), new_copy(c, way, s, -way * s).wait_recv)
                if s < hops(c, way):
                    unless_late(ring.late(c, s + 1), new_copy(c, way, s + 1, -way * s).start)
    for a in range(3):
        pltpu.make_async_copy(landed[a], landed[a], rs_send.at[a]).wait()
    for c, (a, layer) in enumerate(chunks):
        for late in (False, True):
            count = sum(ring.late(c, s) == late for way in WAYS for s in range(1, hops(c, way) + 1))
            unless_late(late, lambda: ring.done(w_out[a], count, ag_send.at[2 * c + late]))


def place(ring, c, way, s):
    a, layer = ring.chunks[c]
    return (a, layer, 0) if s == ring.far else (a, layer, 1 if way == 1 else 2)


def last(ring, *refs):
    w, out = refs[:3], refs[3:6]
    send_sem, recv_sem = refs[6:]
    late = ring.late_hops()
    first = [hop for hop in late if not ring.late(hop[0], hop[2] - 1)]
    then = [hop for hop in late if hop not in first]
    ring.greet()
    ring.greeted()

    def copy(c, way, s):
        a, layer = ring.chunks[c]
        if ring.late(c, s - 1):
            b, *where = place(ring, c, way, s - 1)
            source = out[b].at[*where]
        else:
            source = ring.new(w[a], layer, -way * (s - 1))
        b, *where = place(ring, c, way, s)
        i = then.index((c, way, s + 1)) if (c, way, s + 1) in then else len(then) + WAYS.index(way)
        return ring.send(source, out[b].at[*where], send_sem.at[0], recv_sem.at[i], way)

    @pl.when(ring.waits())
    def _():
        for hop in sorted(first, key=lambda hop: hop[2]):
            copy(*hop).start()
        for c, way, s in then:
            copy(c, way, s - 1).wait_recv()
            copy(c, way, s).start()
        for i, way in enumerate(WAYS):
            ends = [hop for hop in late if hop[1] == way and (*hop[:2], hop[2] + 1) not in then]
            ring.done(w[0], len(ends), recv_sem.at[len(then) + i])
        ring.done(w[0], len(late), send_sem.at[0])


def put(ring, *refs):
    here, there, sem = refs[:9], refs[9:18], refs[18]
    late = {(c, -way * s % ring.n) for c, way, s in ring.late_hops()}

    def whole(i):
        return pltpu.make_async_copy(here[i], there[i], sem.at[i])

    for i in range(3, 9):
        whole(i).start()

    @pl.when(jnp.logical_not(ring.waits()))
    def _():
        for i in range(3):
            whole(i).start()
        for i in range(3):
            whole(i).wait()

    @pl.when(ring.waits())
    def _():
        blocks = [(c, k) for c in range(len(ring.chunks)) for k in range(ring.n) if (c, k) not in late]
        for c, k in blocks:
            a, layer = ring.chunks[c]
            pltpu.make_async_copy(ring.new(here[a], layer, k), ring.new(there[a], layer, k), sem.at[9 + c]).start()
        for c, (a, layer) in enumerate(ring.chunks):
            count = sum(c == other for other, _ in blocks)
            pltpu.make_async_copy(ring.span(here[a], count), ring.span(there[a], count), sem.at[9 + c]).wait()

    for i in range(3, 9):
        whole(i).wait()


def put_last(ring, *refs):
    blocks, _, whole, sem = refs[:3], refs[3:6], refs[6:9], refs[9]

    @pl.when(ring.waits())
    def _():
        for c, way, s in ring.late_hops():
            a, layer, which = place(ring, c, way, s)
            pltpu.make_async_copy(blocks[a].at[layer, which], ring.new(whole[a], layer, -way * s), sem.at[0]).start()
        ring.done(whole[0], len(ring.late_hops()), sem.at[0])


def solution(mesh):
    n = mesh.shape["dp"]

    def step(*arrays):
        terms, weights, m, v = (arrays[i : i + 3] for i in (0, 3, 6, 9))
        ring = Ring(n, weights[0].shape[0])
        blocked = lambda w: w.reshape(ring.layers, n, w.shape[-2] // n, w.shape[-1])
        vmem = lambda x: pltpu.VMEM(x.shape, x.dtype)
        hbm = lambda x: pltpu.HBM(x.shape, x.dtype)
        keep = lambda space, arrays: [pltpu.with_memory_space_constraint(x, space) for x in arrays]
        spec = lambda space, k: [pl.BlockSpec(memory_space=space)] * k
        blocks = [blocked(w) for w in weights]
        arrived = [jax.ShapeDtypeStruct((ring.layers, n - 1, *b.shape[2:]), b.dtype) for b in blocks]
        ends = [jax.ShapeDtypeStruct((ring.layers, 3, *b.shape[2:]), b.dtype) for b in blocks]
        assert len({b.size for b in blocks}) == 1

        out = pl.pallas_call(
            lambda *refs: kernel(ring, *refs),
            name="step",
            out_shape=[vmem(x) for x in (*weights, *m, *v)],
            in_specs=spec(pltpu.HBM, 12),
            out_specs=spec(pltpu.VMEM, 9),
            scratch_shapes=[
                *(pltpu.VMEM(x.shape, x.dtype) for x in (*blocks, *arrived)),
                *(pltpu.SemaphoreType.DMA((k,)) for k in (2 * len(ring.chunks), len(ring.chunks), 7)),
                *(pltpu.SemaphoreType.DMA((k,)) for k in (3, ring.arrivals, 2 * len(ring.chunks), ring.arrivals)),
            ],
            compiler_params=pltpu.CompilerParams(collective_id=0, has_side_effects=True, vmem_limit_bytes=40 << 20),
        )(*keep(pltpu.HBM, [blocked(t[0]) for t in terms] + blocks + [*m, *v]))
        stored = pl.pallas_call(
            lambda *refs: put(ring, *refs),
            name="put",
            out_shape=[hbm(x) for x in out],
            in_specs=spec(pltpu.VMEM, 9),
            out_specs=spec(pltpu.HBM, 9),
            scratch_shapes=[pltpu.SemaphoreType.DMA((9 + len(ring.chunks),))],
            compiler_params=pltpu.CompilerParams(has_side_effects=True, vmem_limit_bytes=20 << 20),
        )(*keep(pltpu.VMEM, out))
        rest = pl.pallas_call(
            lambda *refs: last(ring, *refs),
            name="last",
            out_shape=[vmem(x) for x in ends],
            in_specs=spec(pltpu.VMEM, 3),
            out_specs=spec(pltpu.VMEM, 3),
            scratch_shapes=[pltpu.SemaphoreType.DMA((1,)), pltpu.SemaphoreType.DMA((LATE + 2,))],
            compiler_params=pltpu.CompilerParams(collective_id=1, has_side_effects=True, vmem_limit_bytes=20 << 20),
        )(*keep(pltpu.VMEM, out[:3]))
        whole = pl.pallas_call(
            lambda *refs: put_last(ring, *refs),
            name="put_last",
            out_shape=[hbm(w) for w in weights],
            in_specs=spec(pltpu.VMEM, 3) + spec(pltpu.HBM, 3),
            out_specs=spec(pltpu.HBM, 3),
            input_output_aliases={3: 0, 4: 1, 5: 2},
            scratch_shapes=[pltpu.SemaphoreType.DMA((1,))],
            compiler_params=pltpu.CompilerParams(has_side_effects=True, vmem_limit_bytes=20 << 20),
        )(*keep(pltpu.VMEM, rest), *keep(pltpu.HBM, stored[:3]))
        return (*whole, *stored[3:])

    all_of, cut = P(None, None, None), P(None, "dp", None)
    return jax.shard_map(
        step,
        mesh=mesh,
        in_specs=(P(("rep", "dp"), None, None, None),) * 3 + (all_of,) * 3 + (cut,) * 6,
        out_specs=(P("rep", None, None),) * 3 + (P("rep", "dp", None),) * 6,
        check_vma=False,
    )
```

```python
import jax
import jax.numpy as jnp
from jax import lax
from jax.experimental import pallas as pl
from jax.experimental.pallas import tpu as pltpu
from jax.sharding import PartitionSpec as P

MESH = pl.DeviceIdType.MESH
ROWS = 16
LATE = 2
WAYS = (1, -1)


def adamw(w, m, v, g):
    m = 0.9 * m + 0.1 * g
    v = 0.95 * v + 0.05 * g * g
    step = m * lax.rsqrt(v + 1e-8) + 0.1 * w
    return (w - 0.02 * step).astype(jnp.bfloat16), m, v


class Ring:
    def __init__(self, n, layers):
        self.n, self.layers, self.far = n, layers, n // 2
        self.chunks = [(a, layer) for layer in range(layers) for a in range(3)]
        self.both = [(c, way) for c in range(len(self.chunks)) for way in WAYS]

    def at(self, k):
        return lax.rem(lax.axis_index("dp") + (k + 2 * self.n), self.n)

    def waits(self):
        return lax.rem(lax.axis_index("rep"), 2) == 0

    def hops(self, c, way):
        return self.far if (c % 2 == 0) == (way == 1) else self.n - 1 - self.far

    def slot(self, c, way, s):
        return (0 if way == 1 else self.hops(c, 1)) + s - 1

    def late(self, c, s):
        return s >= self.far - (c >= len(self.chunks) - LATE)

    def late_hops(self):
        return [(c, way, s) for c, way in self.both for s in range(1, self.hops(c, way) + 1) if self.late(c, s)]

    def span(self, ref, count):
        rows = ref.shape[1] // self.n
        if count <= self.n:
            return ref.at[0, pl.ds(0, count * rows)]
        assert count % 2 == 0 and count <= 2 * self.n
        return ref.at[pl.ds(0, 2), pl.ds(0, count // 2 * rows)]

    def done(self, ref, count, sem):
        part = self.span(ref, count)
        pltpu.make_async_copy(part, part, sem).wait()

    def new(self, ref, layer, k):
        rows = ref.shape[1] // self.n
        return ref.at[layer, pl.ds(pl.multiple_of(self.at(k) * rows, ROWS), rows)]

    def greet(self):
        for way in WAYS:
            pl.semaphore_signal(pltpu.get_barrier_semaphore(), inc=1, device_id={"dp": self.at(way)}, device_id_type=MESH)

    def greeted(self):
        pl.semaphore_wait(pltpu.get_barrier_semaphore(), 2)

    def send(self, source, target, send_sem, recv_sem, way):
        return pltpu.make_async_remote_copy(
            src_ref=source, dst_ref=target, send_sem=send_sem, recv_sem=recv_sem, device_id={"dp": self.at(way)}, device_id_type=MESH
        )


def each(rows, body):
    def step(i, _):
        body(pl.ds(pl.multiple_of(i * ROWS, ROWS), ROWS))
        return 0

    lax.fori_loop(0, rows // ROWS, step, 0)


def kernel(ring, *refs):
    refs = iter(refs)
    take = lambda k: [next(refs) for _ in range(k)]
    g_hbm, w_hbm, m_hbm, v_hbm = take(3), take(3), take(3), take(3)
    w_out, m_out, v_out = take(3), take(3), take(3)
    terms, landed = take(3), take(3)
    first_sem, load_sem, own_sem, rs_send, rs_recv, ag_send, ag_recv = refs
    n, far, chunks, at, hops, slot = ring.n, ring.far, ring.chunks, ring.at, ring.hops, ring.slot

    def load(c, k, sem):
        a, layer = chunks[c]
        return pltpu.make_async_copy(g_hbm[a].at[layer, at(k)], terms[a].at[layer, at(k)], sem)

    def first(i):
        c, way = ring.both[i]
        return load(c, way * hops(c, way), first_sem.at[i])

    def others(c):
        return [k for k in range(n) if k not in [way * hops(c, way) % n for way in WAYS]]

    def loaded(c):
        a, layer = chunks[c]
        some = pl.ds(0, len(others(c)))
        pltpu.make_async_copy(g_hbm[a].at[layer, some], terms[a].at[layer, some], load_sem.at[c]).wait()

    ring.greet()
    for i in range(len(ring.both)):
        first(i).start()

    def sum_copy(c, way, s):
        a, layer = chunks[c]
        left = hops(c, way) - s + 1
        source = terms[a].at[layer, at(way * left)] if s == 1 else landed[a].at[layer, slot(c, way, s - 1)]
        return ring.send(source, landed[a].at[layer, slot(c, way, s)], rs_send.at[a], rs_recv.at[c * far + s - 1], way)

    def sums_arrived(c, s):
        a, layer = chunks[c]
        some = landed[a].at[layer, pl.ds(0, sum(s <= hops(c, way) for way in WAYS))]
        pltpu.make_async_copy(some, some, rs_recv.at[c * far + s - 1]).wait()

    def new_copy(c, way, s, k):
        a, layer = chunks[c]
        block = ring.new(w_out[a], layer, k)
        return ring.send(block, block, ag_send.at[2 * c + ring.late(c, s)], ag_recv.at[c * far + s - 1], way)

    def add(c, way, s):
        a, layer = chunks[c]
        sums, mine = landed[a].at[layer, slot(c, way, s)], terms[a].at[layer, at(way * (hops(c, way) - s))]

        def body(rows):
            sums[rows] = (sums[rows].astype(jnp.float32) + mine[rows].astype(jnp.float32)).astype(jnp.bfloat16)

        each(sums.shape[0], body)

    def update(c):
        a, layer = chunks[c]
        one = landed[a].at[layer, slot(c, 1, hops(c, 1))]
        two = landed[a].at[layer, slot(c, -1, hops(c, -1))]
        mine, w, m, v = terms[a].at[layer, at(0)], ring.new(w_out[a], layer, 0), m_out[a].at[layer], v_out[a].at[layer]

        def body(rows):
            g = one[rows].astype(jnp.float32) + two[rows].astype(jnp.float32) + mine[rows].astype(jnp.float32)
            g = g.astype(jnp.bfloat16).astype(jnp.float32)
            w[rows], m[rows], v[rows] = adamw(w[rows].astype(jnp.float32), m[rows], v[rows], g)

        each(one.shape[0], body)

    ring.greeted()
    for i, (c, way) in enumerate(ring.both):
        first(i).wait()
        sum_copy(c, way, 1).start()
    for c, (a, layer) in enumerate(chunks):
        for k in others(c):
            load(c, k, load_sem.at[c]).start()
    for c, (a, layer) in enumerate(chunks):
        pltpu.make_async_copy(w_hbm[a].at[layer, at(0)], ring.new(w_out[a], layer, 0), own_sem.at[0]).start()
    for a in range(3):
        pltpu.make_async_copy(m_hbm[a], m_out[a], own_sem.at[1 + a]).start()
        pltpu.make_async_copy(v_hbm[a], v_out[a], own_sem.at[4 + a]).start()

    for s in range(1, far):
        for c in range(len(chunks)):
            if s == 1:
                loaded(c)
            sums_arrived(c, s)
            for way in WAYS:
                if s < hops(c, way):
                    add(c, way, s)
                    sum_copy(c, way, s + 1).start()
    ring.done(w_out[0], len(chunks), own_sem.at[0])
    for a in range(3):
        pltpu.make_async_copy(m_hbm[a], m_out[a], own_sem.at[1 + a]).wait()
        pltpu.make_async_copy(v_hbm[a], v_out[a], own_sem.at[4 + a]).wait()
    for c in range(len(chunks)):
        sums_arrived(c, far)
        update(c)
        for way in WAYS:
            new_copy(c, way, 1, 0).start()

    def unless_late(late, body):
        if late:
            pl.when(jnp.logical_not(ring.waits()))(body)
        else:
            body()

    for s in range(1, far + 1):
        for c, (a, layer) in enumerate(chunks):
            count = sum(s <= hops(c, way) for way in WAYS)
            unless_late(ring.late(c, s), lambda: ring.done(w_out[a], count, ag_recv.at[c * far + s - 1]))
            for way in WAYS:
                if s < hops(c, way):
                    unless_late(ring.late(c, s + 1), new_copy(c, way, s + 1, -way * s).start)
    for a in range(3):
        pltpu.make_async_copy(landed[a], landed[a], rs_send.at[a]).wait()
    for c, (a, layer) in enumerate(chunks):
        for late in (False, True):
            count = sum(ring.late(c, s) == late for way in WAYS for s in range(1, hops(c, way) + 1))
            unless_late(late, lambda: ring.done(w_out[a], count, ag_send.at[2 * c + late]))


def place(ring, c, way, s):
    a, layer = ring.chunks[c]
    return (a, layer, 0) if s == ring.far else (a, layer, 1 if way == 1 else 2)


def last(ring, *refs):
    w, out = refs[:3], refs[3:6]
    send_sem, recv_sem = refs[6:]
    late = ring.late_hops()
    shared = [(c, way, ring.far) for c, way in ring.both if c == 0]
    first = [hop for hop in late if not ring.late(hop[0], hop[2] - 1) and hop not in shared]
    then = [hop for hop in late if ring.late(hop[0], hop[2] - 1)]
    ring.greet()
    ring.greeted()

    def copy(c, way, s):
        a, layer = ring.chunks[c]
        if ring.late(c, s - 1):
            b, *where = place(ring, c, way, s - 1)
            source = out[b].at[*where]
        else:
            source = ring.new(w[a], layer, -way * (s - 1))
        b, *where = place(ring, c, way, s)
        if (c, way, s) in shared:
            i = shared.index((c, way, s))
            side = source.shape[0] // ROWS * 2 // 5 * ROWS
            rows = pl.ds(0, source.shape[0] - side) if (c, way, s) in late else pl.ds(source.shape[0] - side, side)
            return ring.send(source.at[rows], out[b].at[*where, rows], send_sem.at[2 + i], recv_sem.at[i], way)
        if (c, way, s + 1) in then:
            i = 4 + then.index((c, way, s + 1))
        else:
            i = 2 + WAYS.index(way)
        return ring.send(source, out[b].at[*where], send_sem.at[int((c, way, s) in then)], recv_sem.at[i], way)

    @pl.when(ring.waits())
    def _():
        for hop in sorted(first + shared, key=lambda hop: (hop[2], hop[0])):
            copy(*hop).start()
        for c, way, s in then:
            copy(c, way, s - 1).wait_recv()
            copy(c, way, s).start()
        for i, way in enumerate(WAYS):
            ends = [hop for hop in first + then if hop[1] == way and (*hop[:2], hop[2] + 1) not in then]
            ring.done(w[0], len(ends), recv_sem.at[2 + i])
        ring.done(w[0], len(first), send_sem.at[0])
        ring.done(w[0], len(then), send_sem.at[1])
        for hop in shared:
            copy(*hop).wait()


def put(ring, *refs):
    here, there, sem = refs[:9], refs[9:18], refs[18]
    late = {(c, -way * s % ring.n) for c, way, s in ring.late_hops()}

    def whole(i):
        return pltpu.make_async_copy(here[i], there[i], sem.at[i])

    for i in range(3, 9):
        whole(i).start()

    @pl.when(jnp.logical_not(ring.waits()))
    def _():
        for i in range(3):
            whole(i).start()
        for i in range(3):
            whole(i).wait()

    @pl.when(ring.waits())
    def _():
        blocks = [(c, k) for c in range(len(ring.chunks)) for k in range(ring.n) if (c, k) not in late]
        for c, k in blocks:
            a, layer = ring.chunks[c]
            pltpu.make_async_copy(ring.new(here[a], layer, k), ring.new(there[a], layer, k), sem.at[9 + c]).start()
        for c, (a, layer) in enumerate(ring.chunks):
            count = sum(c == other for other, _ in blocks)
            pltpu.make_async_copy(ring.span(here[a], count), ring.span(there[a], count), sem.at[9 + c]).wait()

    for i in range(3, 9):
        whole(i).wait()


def put_last(ring, *refs):
    blocks, _, whole, sem = refs[:3], refs[3:6], refs[6:9], refs[9]

    @pl.when(ring.waits())
    def _():
        for c, way, s in ring.late_hops():
            a, layer, which = place(ring, c, way, s)
            pltpu.make_async_copy(blocks[a].at[layer, which], ring.new(whole[a], layer, -way * s), sem.at[0]).start()
        ring.done(whole[0], len(ring.late_hops()), sem.at[0])


def solution(mesh):
    n = mesh.shape["dp"]

    def step(*arrays):
        terms, weights, m, v = (arrays[i : i + 3] for i in (0, 3, 6, 9))
        ring = Ring(n, weights[0].shape[0])
        blocked = lambda w: w.reshape(ring.layers, n, w.shape[-2] // n, w.shape[-1])
        vmem = lambda x: pltpu.VMEM(x.shape, x.dtype)
        hbm = lambda x: pltpu.HBM(x.shape, x.dtype)
        keep = lambda space, arrays: [pltpu.with_memory_space_constraint(x, space) for x in arrays]
        spec = lambda space, k: [pl.BlockSpec(memory_space=space)] * k
        blocks = [blocked(w) for w in weights]
        arrived = [jax.ShapeDtypeStruct((ring.layers, n - 1, *b.shape[2:]), b.dtype) for b in blocks]
        ends = [jax.ShapeDtypeStruct((ring.layers, 3, *b.shape[2:]), b.dtype) for b in blocks]
        assert len({b.size for b in blocks}) == 1

        out = pl.pallas_call(
            lambda *refs: kernel(ring, *refs),
            name="step",
            out_shape=[vmem(x) for x in (*weights, *m, *v)],
            in_specs=spec(pltpu.HBM, 12),
            out_specs=spec(pltpu.VMEM, 9),
            scratch_shapes=[
                *(pltpu.VMEM(x.shape, x.dtype) for x in (*blocks, *arrived)),
                *(pltpu.SemaphoreType.DMA((k,)) for k in (2 * len(ring.chunks), len(ring.chunks), 7)),
                *(pltpu.SemaphoreType.DMA((k,)) for k in (3, len(ring.chunks) * ring.far, 2 * len(ring.chunks), len(ring.chunks) * ring.far)),
            ],
            compiler_params=pltpu.CompilerParams(collective_id=0, has_side_effects=True, vmem_limit_bytes=40 << 20),
        )(*keep(pltpu.HBM, [blocked(t[0]) for t in terms] + blocks + [*m, *v]))
        stored = pl.pallas_call(
            lambda *refs: put(ring, *refs),
            name="put",
            out_shape=[hbm(x) for x in out],
            in_specs=spec(pltpu.VMEM, 9),
            out_specs=spec(pltpu.HBM, 9),
            scratch_shapes=[pltpu.SemaphoreType.DMA((9 + len(ring.chunks),))],
            compiler_params=pltpu.CompilerParams(has_side_effects=True, vmem_limit_bytes=20 << 20),
        )(*keep(pltpu.VMEM, out))
        rest = pl.pallas_call(
            lambda *refs: last(ring, *refs),
            name="last",
            out_shape=[vmem(x) for x in ends],
            in_specs=spec(pltpu.VMEM, 3),
            out_specs=spec(pltpu.VMEM, 3),
            scratch_shapes=[pltpu.SemaphoreType.DMA((4,)), pltpu.SemaphoreType.DMA((LATE + 4,))],
            compiler_params=pltpu.CompilerParams(collective_id=1, has_side_effects=True, vmem_limit_bytes=20 << 20),
        )(*keep(pltpu.VMEM, out[:3]))
        whole = pl.pallas_call(
            lambda *refs: put_last(ring, *refs),
            name="put_last",
            out_shape=[hbm(w) for w in weights],
            in_specs=spec(pltpu.VMEM, 3) + spec(pltpu.HBM, 3),
            out_specs=spec(pltpu.HBM, 3),
            input_output_aliases={3: 0, 4: 1, 5: 2},
            scratch_shapes=[pltpu.SemaphoreType.DMA((1,))],
            compiler_params=pltpu.CompilerParams(has_side_effects=True, vmem_limit_bytes=20 << 20),
        )(*keep(pltpu.VMEM, rest), *keep(pltpu.HBM, stored[:3]))
        return (*whole, *stored[3:])

    all_of, cut = P(None, None, None), P(None, "dp", None)
    return jax.shard_map(
        step,
        mesh=mesh,
        in_specs=(P(("rep", "dp"), None, None, None),) * 3 + (all_of,) * 3 + (cut,) * 6,
        out_specs=(P("rep", None, None),) * 3 + (P("rep", "dp", None),) * 6,
        check_vma=False,
    )
```

```python
import jax
import jax.numpy as jnp
from jax import lax
from jax.experimental import pallas as pl
from jax.experimental.pallas import tpu as pltpu
from jax.sharding import PartitionSpec as P

MESH = pl.DeviceIdType.MESH
ROWS = 16
LATE = 2
WAYS = (1, -1)


def adamw(w, m, v, g):
    m = 0.9 * m + 0.1 * g
    v = 0.95 * v + 0.05 * g * g
    step = m * lax.rsqrt(v + 1e-8) + 0.1 * w
    return (w - 0.02 * step).astype(jnp.bfloat16), m, v


class Ring:
    def __init__(self, n, layers):
        self.n, self.layers, self.far = n, layers, n // 2
        self.chunks = [(a, layer) for layer in range(layers) for a in range(3)]
        self.both = [(c, way) for c in range(len(self.chunks)) for way in WAYS]

    def at(self, k):
        return lax.rem(lax.axis_index("dp") + (k + 2 * self.n), self.n)

    def waits(self):
        return lax.rem(lax.axis_index("rep"), 2) == 0

    def hops(self, c, way):
        return self.far if (c % 2 == 0) == (way == 1) else self.n - 1 - self.far

    def slot(self, c, way, s):
        return (0 if way == 1 else self.hops(c, 1)) + s - 1

    def late(self, c, s):
        return s >= self.far - (c >= len(self.chunks) - LATE)

    def late_hops(self):
        return [(c, way, s) for c, way in self.both for s in range(1, self.hops(c, way) + 1) if self.late(c, s)]

    def span(self, ref, count):
        rows = ref.shape[1] // self.n
        if count <= self.n:
            return ref.at[0, pl.ds(0, count * rows)]
        assert count % 2 == 0 and count <= 2 * self.n
        return ref.at[pl.ds(0, 2), pl.ds(0, count // 2 * rows)]

    def done(self, ref, count, sem):
        part = self.span(ref, count)
        pltpu.make_async_copy(part, part, sem).wait()

    def new(self, ref, layer, k):
        rows = ref.shape[1] // self.n
        return ref.at[layer, pl.ds(pl.multiple_of(self.at(k) * rows, ROWS), rows)]

    def greet(self):
        for way in WAYS:
            pl.semaphore_signal(pltpu.get_barrier_semaphore(), inc=1, device_id={"dp": self.at(way)}, device_id_type=MESH)

    def greeted(self):
        pl.semaphore_wait(pltpu.get_barrier_semaphore(), 2)

    def send(self, source, target, send_sem, recv_sem, way):
        return pltpu.make_async_remote_copy(
            src_ref=source, dst_ref=target, send_sem=send_sem, recv_sem=recv_sem, device_id={"dp": self.at(way)}, device_id_type=MESH
        )


def each(rows, body):
    def step(i, _):
        body(pl.ds(pl.multiple_of(i * ROWS, ROWS), ROWS))
        return 0

    lax.fori_loop(0, rows // ROWS, step, 0)


def kernel(ring, *refs):
    refs = iter(refs)
    take = lambda k: [next(refs) for _ in range(k)]
    g_hbm, w_hbm, m_hbm, v_hbm = take(3), take(3), take(3), take(3)
    w_out, m_out, v_out = take(3), take(3), take(3)
    terms, landed = take(3), take(3)
    first_sem, load_sem, own_sem, rs_send, rs_recv, ag_send, ag_recv = refs
    n, far, chunks, at, hops, slot = ring.n, ring.far, ring.chunks, ring.at, ring.hops, ring.slot

    def load(c, k, sem):
        a, layer = chunks[c]
        return pltpu.make_async_copy(g_hbm[a].at[layer, at(k)], terms[a].at[layer, at(k)], sem)

    def first(i):
        c, way = ring.both[i]
        return load(c, way * hops(c, way), first_sem.at[i])

    def others(c):
        return [k for k in range(n) if k not in [way * hops(c, way) % n for way in WAYS]]

    def loaded(c):
        a, layer = chunks[c]
        some = pl.ds(0, len(others(c)))
        pltpu.make_async_copy(g_hbm[a].at[layer, some], terms[a].at[layer, some], load_sem.at[c]).wait()

    ring.greet()
    for i in range(len(ring.both)):
        first(i).start()

    def sum_copy(c, way, s):
        a, layer = chunks[c]
        left = hops(c, way) - s + 1
        source = terms[a].at[layer, at(way * left)] if s == 1 else landed[a].at[layer, slot(c, way, s - 1)]
        return ring.send(source, landed[a].at[layer, slot(c, way, s)], rs_send.at[a], rs_recv.at[c * far + s - 1], way)

    def sums_arrived(c, s):
        a, layer = chunks[c]
        some = landed[a].at[layer, pl.ds(0, sum(s <= hops(c, way) for way in WAYS))]
        pltpu.make_async_copy(some, some, rs_recv.at[c * far + s - 1]).wait()

    def new_copy(c, way, s, k):
        a, layer = chunks[c]
        block = ring.new(w_out[a], layer, k)
        return ring.send(block, block, ag_send.at[2 * c + ring.late(c, s)], ag_recv.at[c * far + s - 1], way)

    def add(c, way, s):
        a, layer = chunks[c]
        sums, mine = landed[a].at[layer, slot(c, way, s)], terms[a].at[layer, at(way * (hops(c, way) - s))]

        def body(rows):
            sums[rows] = (sums[rows].astype(jnp.float32) + mine[rows].astype(jnp.float32)).astype(jnp.bfloat16)

        each(sums.shape[0], body)

    def update(c):
        a, layer = chunks[c]
        one = landed[a].at[layer, slot(c, 1, hops(c, 1))]
        two = landed[a].at[layer, slot(c, -1, hops(c, -1))]
        mine, w, m, v = terms[a].at[layer, at(0)], ring.new(w_out[a], layer, 0), m_out[a].at[layer], v_out[a].at[layer]

        def body(rows):
            g = one[rows].astype(jnp.float32) + two[rows].astype(jnp.float32) + mine[rows].astype(jnp.float32)
            g = g.astype(jnp.bfloat16).astype(jnp.float32)
            w[rows], m[rows], v[rows] = adamw(w[rows].astype(jnp.float32), m[rows], v[rows], g)

        each(one.shape[0], body)

    ring.greeted()
    for i, (c, way) in enumerate(ring.both):
        first(i).wait()
        sum_copy(c, way, 1).start()
    for c, (a, layer) in enumerate(chunks):
        for k in others(c):
            load(c, k, load_sem.at[c]).start()
    for c, (a, layer) in enumerate(chunks):
        pltpu.make_async_copy(w_hbm[a].at[layer, at(0)], ring.new(w_out[a], layer, 0), own_sem.at[0]).start()
    for a in range(3):
        pltpu.make_async_copy(m_hbm[a], m_out[a], own_sem.at[1 + a]).start()
        pltpu.make_async_copy(v_hbm[a], v_out[a], own_sem.at[4 + a]).start()

    for s in range(1, far):
        for c in range(len(chunks)):
            if s == 1:
                loaded(c)
            sums_arrived(c, s)
            for way in WAYS:
                if s < hops(c, way):
                    add(c, way, s)
                    sum_copy(c, way, s + 1).start()
    ring.done(w_out[0], len(chunks), own_sem.at[0])
    for a in range(3):
        pltpu.make_async_copy(m_hbm[a], m_out[a], own_sem.at[1 + a]).wait()
        pltpu.make_async_copy(v_hbm[a], v_out[a], own_sem.at[4 + a]).wait()
    for c in range(len(chunks)):
        sums_arrived(c, far)
        update(c)
        for way in WAYS:
            new_copy(c, way, 1, 0).start()

    def unless_late(late, body):
        if late:
            pl.when(jnp.logical_not(ring.waits()))(body)
        else:
            body()

    for s in range(1, far + 1):
        for c, (a, layer) in enumerate(chunks):
            count = sum(s <= hops(c, way) for way in WAYS)
            unless_late(ring.late(c, s), lambda: ring.done(w_out[a], count, ag_recv.at[c * far + s - 1]))
            for way in WAYS:
                if s < hops(c, way):
                    unless_late(ring.late(c, s + 1), new_copy(c, way, s + 1, -way * s).start)
    for a in range(3):
        pltpu.make_async_copy(landed[a], landed[a], rs_send.at[a]).wait()
    for c, (a, layer) in enumerate(chunks):
        for late in (False, True):
            count = sum(ring.late(c, s) == late for way in WAYS for s in range(1, hops(c, way) + 1))
            unless_late(late, lambda: ring.done(w_out[a], count, ag_send.at[2 * c + late]))


def place(ring, c, way, s):
    a, layer = ring.chunks[c]
    return (a, layer, 0) if s == ring.far else (a, layer, 1 if way == 1 else 2)


def last(ring, *refs):
    w, out = refs[:3], refs[3:6]
    send_sem, recv_sem = refs[6:]
    late = ring.late_hops()
    shared = [(c, way, ring.far) for c, way in ring.both if c == 0]
    first = [hop for hop in late if not ring.late(hop[0], hop[2] - 1) and hop not in shared]
    then = [hop for hop in late if ring.late(hop[0], hop[2] - 1)]
    ring.greet()
    ring.greeted()

    def copy(c, way, s):
        a, layer = ring.chunks[c]
        if ring.late(c, s - 1):
            b, *where = place(ring, c, way, s - 1)
            source = out[b].at[*where]
        else:
            source = ring.new(w[a], layer, -way * (s - 1))
        b, *where = place(ring, c, way, s)
        if (c, way, s) in shared:
            i = shared.index((c, way, s))
            side = source.shape[0] * 3 // 10 // 8 * 8
            rows = pl.ds(0, source.shape[0] - side) if (c, way, s) in late else pl.ds(source.shape[0] - side, side)
            return ring.send(source.at[rows], out[b].at[*where, rows], send_sem.at[2 + i], recv_sem.at[i], way)
        if (c, way, s + 1) in then:
            i = 4 + then.index((c, way, s + 1))
        else:
            i = 2 + WAYS.index(way)
        return ring.send(source, out[b].at[*where], send_sem.at[int((c, way, s) in then)], recv_sem.at[i], way)

    @pl.when(ring.waits())
    def _():
        for hop in sorted(first, key=lambda hop: (hop[2], hop[0])):
            copy(*hop).start()
        for c, way, s in then:
            copy(c, way, s - 1).wait_recv()
            copy(c, way, s).start()
        for hop in shared:
            copy(*hop).start()
        for i, way in enumerate(WAYS):
            ends = [hop for hop in first + then if hop[1] == way and (*hop[:2], hop[2] + 1) not in then]
            ring.done(w[0], len(ends), recv_sem.at[2 + i])
        ring.done(w[0], len(first), send_sem.at[0])
        ring.done(w[0], len(then), send_sem.at[1])
        for hop in shared:
            copy(*hop).wait()


def put(ring, *refs):
    here, there, sem = refs[:9], refs[9:18], refs[18]
    late = {(c, -way * s % ring.n) for c, way, s in ring.late_hops()}

    def whole(i):
        return pltpu.make_async_copy(here[i], there[i], sem.at[i])

    for i in range(3, 9):
        whole(i).start()

    @pl.when(jnp.logical_not(ring.waits()))
    def _():
        for i in range(3):
            whole(i).start()
        for i in range(3):
            whole(i).wait()

    @pl.when(ring.waits())
    def _():
        blocks = [(c, k) for c in range(len(ring.chunks)) for k in range(ring.n) if (c, k) not in late]
        for c, k in blocks:
            a, layer = ring.chunks[c]
            pltpu.make_async_copy(ring.new(here[a], layer, k), ring.new(there[a], layer, k), sem.at[9 + c]).start()
        for c, (a, layer) in enumerate(ring.chunks):
            count = sum(c == other for other, _ in blocks)
            pltpu.make_async_copy(ring.span(here[a], count), ring.span(there[a], count), sem.at[9 + c]).wait()

    for i in range(3, 9):
        whole(i).wait()


def put_last(ring, *refs):
    blocks, _, whole, sem = refs[:3], refs[3:6], refs[6:9], refs[9]

    @pl.when(ring.waits())
    def _():
        for c, way, s in ring.late_hops():
            a, layer, which = place(ring, c, way, s)
            pltpu.make_async_copy(blocks[a].at[layer, which], ring.new(whole[a], layer, -way * s), sem.at[0]).start()
        ring.done(whole[0], len(ring.late_hops()), sem.at[0])


def solution(mesh):
    n = mesh.shape["dp"]

    def step(*arrays):
        terms, weights, m, v = (arrays[i : i + 3] for i in (0, 3, 6, 9))
        ring = Ring(n, weights[0].shape[0])
        blocked = lambda w: w.reshape(ring.layers, n, w.shape[-2] // n, w.shape[-1])
        vmem = lambda x: pltpu.VMEM(x.shape, x.dtype)
        hbm = lambda x: pltpu.HBM(x.shape, x.dtype)
        keep = lambda space, arrays: [pltpu.with_memory_space_constraint(x, space) for x in arrays]
        spec = lambda space, k: [pl.BlockSpec(memory_space=space)] * k
        blocks = [blocked(w) for w in weights]
        arrived = [jax.ShapeDtypeStruct((ring.layers, n - 1, *b.shape[2:]), b.dtype) for b in blocks]
        ends = [jax.ShapeDtypeStruct((ring.layers, 3, *b.shape[2:]), b.dtype) for b in blocks]
        assert len({b.size for b in blocks}) == 1

        out = pl.pallas_call(
            lambda *refs: kernel(ring, *refs),
            name="step",
            out_shape=[vmem(x) for x in (*weights, *m, *v)],
            in_specs=spec(pltpu.HBM, 12),
            out_specs=spec(pltpu.VMEM, 9),
            scratch_shapes=[
                *(pltpu.VMEM(x.shape, x.dtype) for x in (*blocks, *arrived)),
                *(pltpu.SemaphoreType.DMA((k,)) for k in (2 * len(ring.chunks), len(ring.chunks), 7)),
                *(pltpu.SemaphoreType.DMA((k,)) for k in (3, len(ring.chunks) * ring.far, 2 * len(ring.chunks), len(ring.chunks) * ring.far)),
            ],
            compiler_params=pltpu.CompilerParams(collective_id=0, has_side_effects=True, vmem_limit_bytes=40 << 20),
        )(*keep(pltpu.HBM, [blocked(t[0]) for t in terms] + blocks + [*m, *v]))
        stored = pl.pallas_call(
            lambda *refs: put(ring, *refs),
            name="put",
            out_shape=[hbm(x) for x in out],
            in_specs=spec(pltpu.VMEM, 9),
            out_specs=spec(pltpu.HBM, 9),
            scratch_shapes=[pltpu.SemaphoreType.DMA((9 + len(ring.chunks),))],
            compiler_params=pltpu.CompilerParams(has_side_effects=True, vmem_limit_bytes=20 << 20),
        )(*keep(pltpu.VMEM, out))
        rest = pl.pallas_call(
            lambda *refs: last(ring, *refs),
            name="last",
            out_shape=[vmem(x) for x in ends],
            in_specs=spec(pltpu.VMEM, 3),
            out_specs=spec(pltpu.VMEM, 3),
            scratch_shapes=[pltpu.SemaphoreType.DMA((4,)), pltpu.SemaphoreType.DMA((LATE + 4,))],
            compiler_params=pltpu.CompilerParams(collective_id=1, has_side_effects=True, vmem_limit_bytes=20 << 20),
        )(*keep(pltpu.VMEM, out[:3]))
        whole = pl.pallas_call(
            lambda *refs: put_last(ring, *refs),
            name="put_last",
            out_shape=[hbm(w) for w in weights],
            in_specs=spec(pltpu.VMEM, 3) + spec(pltpu.HBM, 3),
            out_specs=spec(pltpu.HBM, 3),
            input_output_aliases={3: 0, 4: 1, 5: 2},
            scratch_shapes=[pltpu.SemaphoreType.DMA((1,))],
            compiler_params=pltpu.CompilerParams(has_side_effects=True, vmem_limit_bytes=20 << 20),
        )(*keep(pltpu.VMEM, rest), *keep(pltpu.HBM, stored[:3]))
        return (*whole, *stored[3:])

    all_of, cut = P(None, None, None), P(None, "dp", None)
    return jax.shard_map(
        step,
        mesh=mesh,
        in_specs=(P(("rep", "dp"), None, None, None),) * 3 + (all_of,) * 3 + (cut,) * 6,
        out_specs=(P("rep", None, None),) * 3 + (P("rep", "dp", None),) * 6,
        check_vma=False,
    )
```

```python
import jax
import jax.numpy as jnp
from jax import lax
from jax.experimental import pallas as pl
from jax.experimental.pallas import tpu as pltpu
from jax.sharding import PartitionSpec as P

MESH = pl.DeviceIdType.MESH
ROWS = 16
LATE = 2
WAYS = (1, -1)


def adamw(w, m, v, g):
    m = 0.9 * m + 0.1 * g
    v = 0.95 * v + 0.05 * g * g
    step = m * lax.rsqrt(v + 1e-8) + 0.1 * w
    return (w - 0.02 * step).astype(jnp.bfloat16), m, v


class Ring:
    def __init__(self, n, layers):
        self.n, self.layers, self.far = n, layers, n // 2
        self.chunks = [(a, layer) for layer in range(layers) for a in range(3)]
        self.both = [(c, way) for c in range(len(self.chunks)) for way in WAYS]

    def at(self, k):
        return lax.rem(lax.axis_index("dp") + (k + 2 * self.n), self.n)

    def waits(self):
        return lax.rem(lax.axis_index("rep"), 2) == 0

    def hops(self, c, way):
        return self.far if (c % 2 == 0) == (way == 1) else self.n - 1 - self.far

    def slot(self, c, way, s):
        return (0 if way == 1 else self.hops(c, 1)) + s - 1

    def late(self, c, s):
        return s >= self.far - (c >= len(self.chunks) - LATE)

    def late_hops(self):
        return [(c, way, s) for c, way in self.both for s in range(1, self.hops(c, way) + 1) if self.late(c, s)]

    def span(self, ref, count):
        rows = ref.shape[1] // self.n
        if count <= self.n:
            return ref.at[0, pl.ds(0, count * rows)]
        assert count % 2 == 0 and count <= 2 * self.n
        return ref.at[pl.ds(0, 2), pl.ds(0, count // 2 * rows)]

    def done(self, ref, count, sem):
        part = self.span(ref, count)
        pltpu.make_async_copy(part, part, sem).wait()

    def new(self, ref, layer, k):
        rows = ref.shape[1] // self.n
        return ref.at[layer, pl.ds(pl.multiple_of(self.at(k) * rows, ROWS), rows)]

    def greet(self):
        for way in WAYS:
            pl.semaphore_signal(pltpu.get_barrier_semaphore(), inc=1, device_id={"dp": self.at(way)}, device_id_type=MESH)

    def greeted(self):
        pl.semaphore_wait(pltpu.get_barrier_semaphore(), 2)

    def send(self, source, target, send_sem, recv_sem, way):
        return pltpu.make_async_remote_copy(
            src_ref=source, dst_ref=target, send_sem=send_sem, recv_sem=recv_sem, device_id={"dp": self.at(way)}, device_id_type=MESH
        )


def each(rows, body):
    def step(i, _):
        body(pl.ds(pl.multiple_of(i * ROWS, ROWS), ROWS))
        return 0

    lax.fori_loop(0, rows // ROWS, step, 0)


def kernel(ring, *refs):
    refs = iter(refs)
    take = lambda k: [next(refs) for _ in range(k)]
    g_hbm, w_hbm, m_hbm, v_hbm = take(3), take(3), take(3), take(3)
    w_out, m_out, v_out = take(3), take(3), take(3)
    terms, landed = take(3), take(3)
    load_sem, own_sem, rs_send, rs_recv, ag_send, ag_recv = refs
    n, far, chunks, at, hops, slot = ring.n, ring.far, ring.chunks, ring.at, ring.hops, ring.slot

    def load(c, k, sem):
        a, layer = chunks[c]
        return pltpu.make_async_copy(g_hbm[a].at[layer, at(k)], terms[a].at[layer, at(k)], sem)

    def others(c):
        return [k for k in range(n) if k not in [way * hops(c, way) % n for way in WAYS]]

    def loaded(c):
        a, layer = chunks[c]
        some = pl.ds(0, len(others(c)))
        pltpu.make_async_copy(g_hbm[a].at[layer, some], terms[a].at[layer, some], load_sem.at[c]).wait()

    ring.greet()

    def sum_copy(c, way, s):
        a, layer = chunks[c]
        left = hops(c, way) - s + 1
        source = g_hbm[a].at[layer, at(way * left)] if s == 1 else landed[a].at[layer, slot(c, way, s - 1)]
        return ring.send(source, landed[a].at[layer, slot(c, way, s)], rs_send.at[a], rs_recv.at[c * far + s - 1], way)

    def sums_arrived(c, s):
        a, layer = chunks[c]
        some = landed[a].at[layer, pl.ds(0, sum(s <= hops(c, way) for way in WAYS))]
        pltpu.make_async_copy(some, some, rs_recv.at[c * far + s - 1]).wait()

    def new_copy(c, way, s, k):
        a, layer = chunks[c]
        block = ring.new(w_out[a], layer, k)
        return ring.send(block, block, ag_send.at[2 * c + ring.late(c, s)], ag_recv.at[c * far + s - 1], way)

    def add(c, way, s):
        a, layer = chunks[c]
        sums, mine = landed[a].at[layer, slot(c, way, s)], terms[a].at[layer, at(way * (hops(c, way) - s))]

        def body(rows):
            sums[rows] = (sums[rows].astype(jnp.float32) + mine[rows].astype(jnp.float32)).astype(jnp.bfloat16)

        each(sums.shape[0], body)

    def update(c):
        a, layer = chunks[c]
        one = landed[a].at[layer, slot(c, 1, hops(c, 1))]
        two = landed[a].at[layer, slot(c, -1, hops(c, -1))]
        mine, w, m, v = terms[a].at[layer, at(0)], ring.new(w_out[a], layer, 0), m_out[a].at[layer], v_out[a].at[layer]

        def body(rows):
            g = one[rows].astype(jnp.float32) + two[rows].astype(jnp.float32) + mine[rows].astype(jnp.float32)
            g = g.astype(jnp.bfloat16).astype(jnp.float32)
            w[rows], m[rows], v[rows] = adamw(w[rows].astype(jnp.float32), m[rows], v[rows], g)

        each(one.shape[0], body)

    ring.greeted()
    for c, way in ring.both:
        sum_copy(c, way, 1).start()
    for c, (a, layer) in enumerate(chunks):
        for k in others(c):
            load(c, k, load_sem.at[c]).start()
    for c, (a, layer) in enumerate(chunks):
        pltpu.make_async_copy(w_hbm[a].at[layer, at(0)], ring.new(w_out[a], layer, 0), own_sem.at[0]).start()
    for a in range(3):
        pltpu.make_async_copy(m_hbm[a], m_out[a], own_sem.at[1 + a]).start()
        pltpu.make_async_copy(v_hbm[a], v_out[a], own_sem.at[4 + a]).start()

    for s in range(1, far):
        for c in range(len(chunks)):
            if s == 1:
                loaded(c)
            sums_arrived(c, s)
            for way in WAYS:
                if s < hops(c, way):
                    add(c, way, s)
                    sum_copy(c, way, s + 1).start()
    ring.done(w_out[0], len(chunks), own_sem.at[0])
    for a in range(3):
        pltpu.make_async_copy(m_hbm[a], m_out[a], own_sem.at[1 + a]).wait()
        pltpu.make_async_copy(v_hbm[a], v_out[a], own_sem.at[4 + a]).wait()
    for c in range(len(chunks)):
        sums_arrived(c, far)
        update(c)
        for way in WAYS:
            new_copy(c, way, 1, 0).start()

    def unless_late(late, body):
        if late:
            pl.when(jnp.logical_not(ring.waits()))(body)
        else:
            body()

    for s in range(1, far + 1):
        for c, (a, layer) in enumerate(chunks):
            count = sum(s <= hops(c, way) for way in WAYS)
            unless_late(ring.late(c, s), lambda: ring.done(w_out[a], count, ag_recv.at[c * far + s - 1]))
            for way in WAYS:
                if s < hops(c, way):
                    unless_late(ring.late(c, s + 1), new_copy(c, way, s + 1, -way * s).start)
    for a in range(3):
        pltpu.make_async_copy(landed[a], landed[a], rs_send.at[a]).wait()
    for c, (a, layer) in enumerate(chunks):
        for late in (False, True):
            count = sum(ring.late(c, s) == late for way in WAYS for s in range(1, hops(c, way) + 1))
            unless_late(late, lambda: ring.done(w_out[a], count, ag_send.at[2 * c + late]))


def place(ring, c, way, s):
    a, layer = ring.chunks[c]
    return (a, layer, 0) if s == ring.far else (a, layer, 1 if way == 1 else 2)


def last(ring, *refs):
    w, out = refs[:3], refs[3:6]
    send_sem, recv_sem = refs[6:]
    late = ring.late_hops()
    shared = [(c, way, ring.far) for c, way in ring.both if c == 0]
    first = [hop for hop in late if not ring.late(hop[0], hop[2] - 1) and hop not in shared]
    then = [hop for hop in late if ring.late(hop[0], hop[2] - 1)]
    ring.greet()
    ring.greeted()

    def copy(c, way, s):
        a, layer = ring.chunks[c]
        if ring.late(c, s - 1):
            b, *where = place(ring, c, way, s - 1)
            source = out[b].at[*where]
        else:
            source = ring.new(w[a], layer, -way * (s - 1))
        b, *where = place(ring, c, way, s)
        if (c, way, s) in shared:
            i = shared.index((c, way, s))
            side = source.shape[0] * 3 // 10 // 8 * 8
            rows = pl.ds(0, source.shape[0] - side) if (c, way, s) in late else pl.ds(source.shape[0] - side, side)
            return ring.send(source.at[rows], out[b].at[*where, rows], send_sem.at[2 + i], recv_sem.at[i], way)
        if (c, way, s + 1) in then:
            i = 4 + then.index((c, way, s + 1))
        else:
            i = 2 + WAYS.index(way)
        return ring.send(source, out[b].at[*where], send_sem.at[int((c, way, s) in then)], recv_sem.at[i], way)

    @pl.when(ring.waits())
    def _():
        for hop in sorted(first, key=lambda hop: (hop[2], hop[0])):
            copy(*hop).start()
        for c, way, s in then:
            copy(c, way, s - 1).wait_recv()
            copy(c, way, s).start()
        for hop in shared:
            copy(*hop).start()
        for i, way in enumerate(WAYS):
            ends = [hop for hop in first + then if hop[1] == way and (*hop[:2], hop[2] + 1) not in then]
            ring.done(w[0], len(ends), recv_sem.at[2 + i])
        ring.done(w[0], len(first), send_sem.at[0])
        ring.done(w[0], len(then), send_sem.at[1])
        for hop in shared:
            copy(*hop).wait()


def put(ring, *refs):
    here, there, sem = refs[:9], refs[9:18], refs[18]
    late = {(c, -way * s % ring.n) for c, way, s in ring.late_hops()}

    def whole(i):
        return pltpu.make_async_copy(here[i], there[i], sem.at[i])

    for i in range(3, 9):
        whole(i).start()

    @pl.when(jnp.logical_not(ring.waits()))
    def _():
        for i in range(3):
            whole(i).start()
        for i in range(3):
            whole(i).wait()

    @pl.when(ring.waits())
    def _():
        blocks = [(c, k) for c in range(len(ring.chunks)) for k in range(ring.n) if (c, k) not in late]
        for c, k in blocks:
            a, layer = ring.chunks[c]
            pltpu.make_async_copy(ring.new(here[a], layer, k), ring.new(there[a], layer, k), sem.at[9 + c]).start()
        for c, (a, layer) in enumerate(ring.chunks):
            count = sum(c == other for other, _ in blocks)
            pltpu.make_async_copy(ring.span(here[a], count), ring.span(there[a], count), sem.at[9 + c]).wait()

    for i in range(3, 9):
        whole(i).wait()


def put_last(ring, *refs):
    blocks, _, whole, sem = refs[:3], refs[3:6], refs[6:9], refs[9]

    @pl.when(ring.waits())
    def _():
        for c, way, s in ring.late_hops():
            a, layer, which = place(ring, c, way, s)
            pltpu.make_async_copy(blocks[a].at[layer, which], ring.new(whole[a], layer, -way * s), sem.at[0]).start()
        ring.done(whole[0], len(ring.late_hops()), sem.at[0])


def solution(mesh):
    n = mesh.shape["dp"]

    def step(*arrays):
        terms, weights, m, v = (arrays[i : i + 3] for i in (0, 3, 6, 9))
        ring = Ring(n, weights[0].shape[0])
        blocked = lambda w: w.reshape(ring.layers, n, w.shape[-2] // n, w.shape[-1])
        vmem = lambda x: pltpu.VMEM(x.shape, x.dtype)
        hbm = lambda x: pltpu.HBM(x.shape, x.dtype)
        keep = lambda space, arrays: [pltpu.with_memory_space_constraint(x, space) for x in arrays]
        spec = lambda space, k: [pl.BlockSpec(memory_space=space)] * k
        blocks = [blocked(w) for w in weights]
        arrived = [jax.ShapeDtypeStruct((ring.layers, n - 1, *b.shape[2:]), b.dtype) for b in blocks]
        ends = [jax.ShapeDtypeStruct((ring.layers, 3, *b.shape[2:]), b.dtype) for b in blocks]
        assert len({b.size for b in blocks}) == 1

        out = pl.pallas_call(
            lambda *refs: kernel(ring, *refs),
            name="step",
            out_shape=[vmem(x) for x in (*weights, *m, *v)],
            in_specs=spec(pltpu.HBM, 12),
            out_specs=spec(pltpu.VMEM, 9),
            scratch_shapes=[
                *(pltpu.VMEM(x.shape, x.dtype) for x in (*blocks, *arrived)),
                *(pltpu.SemaphoreType.DMA((k,)) for k in (len(ring.chunks), 7)),
                *(pltpu.SemaphoreType.DMA((k,)) for k in (3, len(ring.chunks) * ring.far, 2 * len(ring.chunks), len(ring.chunks) * ring.far)),
            ],
            compiler_params=pltpu.CompilerParams(collective_id=0, has_side_effects=True, vmem_limit_bytes=40 << 20),
        )(*keep(pltpu.HBM, [blocked(t[0]) for t in terms] + blocks + [*m, *v]))
        stored = pl.pallas_call(
            lambda *refs: put(ring, *refs),
            name="put",
            out_shape=[hbm(x) for x in out],
            in_specs=spec(pltpu.VMEM, 9),
            out_specs=spec(pltpu.HBM, 9),
            scratch_shapes=[pltpu.SemaphoreType.DMA((9 + len(ring.chunks),))],
            compiler_params=pltpu.CompilerParams(has_side_effects=True, vmem_limit_bytes=20 << 20),
        )(*keep(pltpu.VMEM, out))
        rest = pl.pallas_call(
            lambda *refs: last(ring, *refs),
            name="last",
            out_shape=[vmem(x) for x in ends],
            in_specs=spec(pltpu.VMEM, 3),
            out_specs=spec(pltpu.VMEM, 3),
            scratch_shapes=[pltpu.SemaphoreType.DMA((4,)), pltpu.SemaphoreType.DMA((LATE + 4,))],
            compiler_params=pltpu.CompilerParams(collective_id=1, has_side_effects=True, vmem_limit_bytes=20 << 20),
        )(*keep(pltpu.VMEM, out[:3]))
        whole = pl.pallas_call(
            lambda *refs: put_last(ring, *refs),
            name="put_last",
            out_shape=[hbm(w) for w in weights],
            in_specs=spec(pltpu.VMEM, 3) + spec(pltpu.HBM, 3),
            out_specs=spec(pltpu.HBM, 3),
            input_output_aliases={3: 0, 4: 1, 5: 2},
            scratch_shapes=[pltpu.SemaphoreType.DMA((1,))],
            compiler_params=pltpu.CompilerParams(has_side_effects=True, vmem_limit_bytes=20 << 20),
        )(*keep(pltpu.VMEM, rest), *keep(pltpu.HBM, stored[:3]))
        return (*whole, *stored[3:])

    all_of, cut = P(None, None, None), P(None, "dp", None)
    return jax.shard_map(
        step,
        mesh=mesh,
        in_specs=(P(("rep", "dp"), None, None, None),) * 3 + (all_of,) * 3 + (cut,) * 6,
        out_specs=(P("rep", None, None),) * 3 + (P("rep", "dp", None),) * 6,
        check_vma=False,
    )
```

```python
import jax
import jax.numpy as jnp
from jax import lax
from jax.experimental import pallas as pl
from jax.experimental.pallas import tpu as pltpu
from jax.sharding import PartitionSpec as P

MESH = pl.DeviceIdType.MESH
ROWS = 16
LATE = 2
WAYS = (1, -1)


def adamw(w, m, v, g):
    m = 0.9 * m + 0.1 * g
    v = 0.95 * v + 0.05 * g * g
    step = m * lax.rsqrt(v + 1e-8) + 0.1 * w
    return (w - 0.02 * step).astype(jnp.bfloat16), m, v


class Ring:
    def __init__(self, n, layers):
        self.n, self.layers, self.far = n, layers, n // 2
        self.chunks = [(a, layer) for layer in range(layers) for a in range(3)]
        self.both = [(c, way) for c in range(len(self.chunks)) for way in WAYS]

    def at(self, k):
        return lax.rem(lax.axis_index("dp") + (k + 2 * self.n), self.n)

    def waits(self):
        return lax.rem(lax.axis_index("rep"), 2) == 0

    def hops(self, c, way):
        return self.far if (c % 2 == 0) == (way == 1) else self.n - 1 - self.far

    def slot(self, c, way, s):
        return (0 if way == 1 else self.hops(c, 1)) + s - 1

    def late(self, c, s):
        return s >= self.far - (c >= len(self.chunks) - LATE)

    def late_hops(self):
        return [(c, way, s) for c, way in self.both for s in range(1, self.hops(c, way) + 1) if self.late(c, s)]

    def span(self, ref, count):
        rows = ref.shape[1] // self.n
        if count <= self.n:
            return ref.at[0, pl.ds(0, count * rows)]
        assert count % 2 == 0 and count <= 2 * self.n
        return ref.at[pl.ds(0, 2), pl.ds(0, count // 2 * rows)]

    def done(self, ref, count, sem):
        part = self.span(ref, count)
        pltpu.make_async_copy(part, part, sem).wait()

    def new(self, ref, layer, k):
        rows = ref.shape[1] // self.n
        return ref.at[layer, pl.ds(pl.multiple_of(self.at(k) * rows, ROWS), rows)]

    def greet(self):
        for way in WAYS:
            pl.semaphore_signal(pltpu.get_barrier_semaphore(), inc=1, device_id={"dp": self.at(way)}, device_id_type=MESH)

    def greeted(self):
        pl.semaphore_wait(pltpu.get_barrier_semaphore(), 2)

    def send(self, source, target, send_sem, recv_sem, way):
        return pltpu.make_async_remote_copy(
            src_ref=source, dst_ref=target, send_sem=send_sem, recv_sem=recv_sem, device_id={"dp": self.at(way)}, device_id_type=MESH
        )


def each(rows, body):
    def step(i, _):
        body(pl.ds(pl.multiple_of(i * ROWS, ROWS), ROWS))
        return 0

    lax.fori_loop(0, rows // ROWS, step, 0)


def kernel(ring, *refs):
    refs = iter(refs)
    take = lambda k: [next(refs) for _ in range(k)]
    g_hbm, w_hbm, m_hbm, v_hbm = take(3), take(3), take(3), take(3)
    w_out, m_out, v_out = take(3), take(3), take(3)
    terms, landed = take(3), take(3)
    load_sem, own_sem, rs_send, rs_recv, ag_send, ag_recv = refs
    n, far, chunks, at, hops, slot = ring.n, ring.far, ring.chunks, ring.at, ring.hops, ring.slot

    def load(c, k, sem):
        a, layer = chunks[c]
        return pltpu.make_async_copy(g_hbm[a].at[layer, at(k)], terms[a].at[layer, at(k)], sem)

    def others(c):
        return [k for k in range(n) if k not in [way * hops(c, way) % n for way in WAYS]]

    def loaded(c):
        a, layer = chunks[c]
        some = pl.ds(0, len(others(c)))
        pltpu.make_async_copy(g_hbm[a].at[layer, some], terms[a].at[layer, some], load_sem.at[c]).wait()

    ring.greet()

    def sum_copy(c, way, s):
        a, layer = chunks[c]
        left = hops(c, way) - s + 1
        source = g_hbm[a].at[layer, at(way * left)] if s == 1 else landed[a].at[layer, slot(c, way, s - 1)]
        return ring.send(source, landed[a].at[layer, slot(c, way, s)], rs_send.at[a], rs_recv.at[c * far + s - 1], way)

    def sums_arrived(c, s):
        a, layer = chunks[c]
        some = landed[a].at[layer, pl.ds(0, sum(s <= hops(c, way) for way in WAYS))]
        pltpu.make_async_copy(some, some, rs_recv.at[c * far + s - 1]).wait()

    def new_copy(c, way, s, k):
        a, layer = chunks[c]
        block = ring.new(w_out[a], layer, k)
        return ring.send(block, block, ag_send.at[2 * c + ring.late(c, s)], ag_recv.at[c * far + s - 1], way)

    def add(c, way, s):
        a, layer = chunks[c]
        sums, mine = landed[a].at[layer, slot(c, way, s)], terms[a].at[layer, at(way * (hops(c, way) - s))]

        def body(rows):
            sums[rows] = (sums[rows].astype(jnp.float32) + mine[rows].astype(jnp.float32)).astype(jnp.bfloat16)

        each(sums.shape[0], body)

    def update(c):
        a, layer = chunks[c]
        one = landed[a].at[layer, slot(c, 1, hops(c, 1))]
        two = landed[a].at[layer, slot(c, -1, hops(c, -1))]
        mine, w, m, v = terms[a].at[layer, at(0)], ring.new(w_out[a], layer, 0), m_out[a].at[layer], v_out[a].at[layer]

        def body(rows):
            g = one[rows].astype(jnp.float32) + two[rows].astype(jnp.float32) + mine[rows].astype(jnp.float32)
            g = g.astype(jnp.bfloat16).astype(jnp.float32)
            w[rows], m[rows], v[rows] = adamw(w[rows].astype(jnp.float32), m[rows], v[rows], g)

        each(one.shape[0], body)

    ring.greeted()
    for c, way in ring.both:
        sum_copy(c, way, 1).start()
    for c, (a, layer) in enumerate(chunks):
        for k in others(c):
            load(c, k, load_sem.at[c]).start()
    for c, (a, layer) in enumerate(chunks):
        pltpu.make_async_copy(w_hbm[a].at[layer, at(0)], ring.new(w_out[a], layer, 0), own_sem.at[0]).start()
    for a in range(3):
        pltpu.make_async_copy(m_hbm[a], m_out[a], own_sem.at[1 + a]).start()
        pltpu.make_async_copy(v_hbm[a], v_out[a], own_sem.at[4 + a]).start()

    for s in range(1, far):
        for c in range(len(chunks)):
            if s == 1:
                loaded(c)
            sums_arrived(c, s)
            for way in WAYS:
                if s < hops(c, way):
                    add(c, way, s)
                    sum_copy(c, way, s + 1).start()
    ring.done(w_out[0], len(chunks), own_sem.at[0])
    for a in range(3):
        pltpu.make_async_copy(m_hbm[a], m_out[a], own_sem.at[1 + a]).wait()
        pltpu.make_async_copy(v_hbm[a], v_out[a], own_sem.at[4 + a]).wait()
    for c in range(len(chunks)):
        sums_arrived(c, far)
        update(c)
        for way in WAYS:
            new_copy(c, way, 1, 0).start()

    def unless_late(late, body):
        if late:
            pl.when(jnp.logical_not(ring.waits()))(body)
        else:
            body()

    for s in range(1, far + 1):
        for c, (a, layer) in enumerate(chunks):
            count = sum(s <= hops(c, way) for way in WAYS)
            unless_late(ring.late(c, s), lambda: ring.done(w_out[a], count, ag_recv.at[c * far + s - 1]))
            for way in WAYS:
                if s < hops(c, way):
                    unless_late(ring.late(c, s + 1), new_copy(c, way, s + 1, -way * s).start)
    for a in range(3):
        pltpu.make_async_copy(landed[a], landed[a], rs_send.at[a]).wait()
    for c, (a, layer) in enumerate(chunks):
        for late in (False, True):
            count = sum(ring.late(c, s) == late for way in WAYS for s in range(1, hops(c, way) + 1))
            unless_late(late, lambda: ring.done(w_out[a], count, ag_send.at[2 * c + late]))


def place(ring, c, way, s):
    a, layer = ring.chunks[c]
    return (a, layer, 0) if s == ring.far else (a, layer, 1 if way == 1 else 2)


def last(ring, *refs):
    w, out = refs[:3], refs[3:6]
    send_sem, recv_sem = refs[6:]
    late = ring.late_hops()
    shared = [(c, way, ring.far) for c, way in ring.both if c == 0]
    first = [hop for hop in late if not ring.late(hop[0], hop[2] - 1) and hop not in shared]
    then = [hop for hop in late if ring.late(hop[0], hop[2] - 1)]
    ring.greet()
    ring.greeted()

    def copy(c, way, s):
        a, layer = ring.chunks[c]
        if ring.late(c, s - 1):
            b, *where = place(ring, c, way, s - 1)
            source = out[b].at[*where]
        else:
            source = ring.new(w[a], layer, -way * (s - 1))
        b, *where = place(ring, c, way, s)
        if (c, way, s) in shared:
            side = source.shape[0] * 3 // 10 // 8 * 8
            rows = pl.ds(0, source.shape[0] - side) if (c, way, s) in late else pl.ds(source.shape[0] - side, side)
            return ring.send(source.at[rows], out[b].at[*where, rows], send_sem.at[0], recv_sem.at[0], way)
        if (c, way, s + 1) in then:
            i = 1 + then.index((c, way, s + 1))
        else:
            i = 0
        return ring.send(source, out[b].at[*where], send_sem.at[0], recv_sem.at[i], way)

    @pl.when(ring.waits())
    def _():
        for hop in sorted(first, key=lambda hop: (hop[2], hop[0])):
            copy(*hop).start()
        for c, way, s in then:
            copy(c, way, s - 1).wait_recv()
            copy(c, way, s).start()
        for hop in shared:
            copy(*hop).start()
        ring.done(w[0], len(late) - len(then), recv_sem.at[0])
        ring.done(w[0], len(late), send_sem.at[0])


def put(ring, *refs):
    here, there, sem = refs[:9], refs[9:18], refs[18]
    late = {(c, -way * s % ring.n) for c, way, s in ring.late_hops()}

    def whole(i):
        return pltpu.make_async_copy(here[i], there[i], sem.at[i])

    for i in range(3, 9):
        whole(i).start()

    @pl.when(jnp.logical_not(ring.waits()))
    def _():
        for i in range(3):
            whole(i).start()
        for i in range(3):
            whole(i).wait()

    @pl.when(ring.waits())
    def _():
        blocks = [(c, k) for c in range(len(ring.chunks)) for k in range(ring.n) if (c, k) not in late]
        for c, k in blocks:
            a, layer = ring.chunks[c]
            pltpu.make_async_copy(ring.new(here[a], layer, k), ring.new(there[a], layer, k), sem.at[9 + c]).start()
        for c, (a, layer) in enumerate(ring.chunks):
            count = sum(c == other for other, _ in blocks)
            pltpu.make_async_copy(ring.span(here[a], count), ring.span(there[a], count), sem.at[9 + c]).wait()

    for i in range(3, 9):
        whole(i).wait()


def put_last(ring, *refs):
    blocks, _, whole, sem = refs[:3], refs[3:6], refs[6:9], refs[9]

    @pl.when(ring.waits())
    def _():
        for c, way, s in ring.late_hops():
            a, layer, which = place(ring, c, way, s)
            pltpu.make_async_copy(blocks[a].at[layer, which], ring.new(whole[a], layer, -way * s), sem.at[0]).start()
        ring.done(whole[0], len(ring.late_hops()), sem.at[0])


def solution(mesh):
    n = mesh.shape["dp"]

    def step(*arrays):
        terms, weights, m, v = (arrays[i : i + 3] for i in (0, 3, 6, 9))
        ring = Ring(n, weights[0].shape[0])
        blocked = lambda w: w.reshape(ring.layers, n, w.shape[-2] // n, w.shape[-1])
        vmem = lambda x: pltpu.VMEM(x.shape, x.dtype)
        hbm = lambda x: pltpu.HBM(x.shape, x.dtype)
        keep = lambda space, arrays: [pltpu.with_memory_space_constraint(x, space) for x in arrays]
        spec = lambda space, k: [pl.BlockSpec(memory_space=space)] * k
        blocks = [blocked(w) for w in weights]
        arrived = [jax.ShapeDtypeStruct((ring.layers, n - 1, *b.shape[2:]), b.dtype) for b in blocks]
        ends = [jax.ShapeDtypeStruct((ring.layers, 3, *b.shape[2:]), b.dtype) for b in blocks]
        assert len({b.size for b in blocks}) == 1

        out = pl.pallas_call(
            lambda *refs: kernel(ring, *refs),
            name="step",
            out_shape=[vmem(x) for x in (*weights, *m, *v)],
            in_specs=spec(pltpu.HBM, 12),
            out_specs=spec(pltpu.VMEM, 9),
            scratch_shapes=[
                *(pltpu.VMEM(x.shape, x.dtype) for x in (*blocks, *arrived)),
                *(pltpu.SemaphoreType.DMA((k,)) for k in (len(ring.chunks), 7)),
                *(pltpu.SemaphoreType.DMA((k,)) for k in (3, len(ring.chunks) * ring.far, 2 * len(ring.chunks), len(ring.chunks) * ring.far)),
            ],
            compiler_params=pltpu.CompilerParams(collective_id=0, has_side_effects=True, vmem_limit_bytes=40 << 20),
        )(*keep(pltpu.HBM, [blocked(t[0]) for t in terms] + blocks + [*m, *v]))
        stored = pl.pallas_call(
            lambda *refs: put(ring, *refs),
            name="put",
            out_shape=[hbm(x) for x in out],
            in_specs=spec(pltpu.VMEM, 9),
            out_specs=spec(pltpu.HBM, 9),
            scratch_shapes=[pltpu.SemaphoreType.DMA((9 + len(ring.chunks),))],
            compiler_params=pltpu.CompilerParams(has_side_effects=True, vmem_limit_bytes=20 << 20),
        )(*keep(pltpu.VMEM, out))
        rest = pl.pallas_call(
            lambda *refs: last(ring, *refs),
            name="last",
            out_shape=[vmem(x) for x in ends],
            in_specs=spec(pltpu.VMEM, 3),
            out_specs=spec(pltpu.VMEM, 3),
            scratch_shapes=[pltpu.SemaphoreType.DMA((1,)), pltpu.SemaphoreType.DMA((LATE + 1,))],
            compiler_params=pltpu.CompilerParams(collective_id=1, has_side_effects=True, vmem_limit_bytes=20 << 20),
        )(*keep(pltpu.VMEM, out[:3]))
        whole = pl.pallas_call(
            lambda *refs: put_last(ring, *refs),
            name="put_last",
            out_shape=[hbm(w) for w in weights],
            in_specs=spec(pltpu.VMEM, 3) + spec(pltpu.HBM, 3),
            out_specs=spec(pltpu.HBM, 3),
            input_output_aliases={3: 0, 4: 1, 5: 2},
            scratch_shapes=[pltpu.SemaphoreType.DMA((1,))],
            compiler_params=pltpu.CompilerParams(has_side_effects=True, vmem_limit_bytes=20 << 20),
        )(*keep(pltpu.VMEM, rest), *keep(pltpu.HBM, stored[:3]))
        return (*whole, *stored[3:])

    all_of, cut = P(None, None, None), P(None, "dp", None)
    return jax.shard_map(
        step,
        mesh=mesh,
        in_specs=(P(("rep", "dp"), None, None, None),) * 3 + (all_of,) * 3 + (cut,) * 6,
        out_specs=(P("rep", None, None),) * 3 + (P("rep", "dp", None),) * 6,
        check_vma=False,
    )
```

```python
import jax
import jax.numpy as jnp
from jax import lax
from jax.experimental import pallas as pl
from jax.experimental.pallas import tpu as pltpu
from jax.sharding import PartitionSpec as P

MESH = pl.DeviceIdType.MESH
ROWS = 16
LATE = 2
WAYS = (1, -1)


def adamw(w, m, v, g):
    m = 0.9 * m + 0.1 * g
    v = 0.95 * v + 0.05 * g * g
    step = m * lax.rsqrt(v + 1e-8) + 0.1 * w
    return (w - 0.02 * step).astype(jnp.bfloat16), m, v


class Ring:
    def __init__(self, n, layers):
        self.n, self.layers, self.far = n, layers, n // 2
        self.chunks = [(a, layer) for layer in range(layers) for a in range(3)]
        self.both = [(c, way) for c in range(len(self.chunks)) for way in WAYS]

    def at(self, k):
        return lax.rem(lax.axis_index("dp") + (k + 2 * self.n), self.n)

    def waits(self):
        return lax.rem(lax.axis_index("rep"), 2) == 0

    def hops(self, c, way):
        return self.far if (c % 2 == 0) == (way == 1) else self.n - 1 - self.far

    def slot(self, c, way, s):
        return (0 if way == 1 else self.hops(c, 1)) + s - 1

    def late(self, c, s):
        return s >= self.far - (c >= len(self.chunks) - LATE)

    def late_hops(self):
        return [(c, way, s) for c, way in self.both for s in range(1, self.hops(c, way) + 1) if self.late(c, s)]

    def span(self, ref, count):
        rows = ref.shape[1] // self.n
        if count <= self.n:
            return ref.at[0, pl.ds(0, count * rows)]
        assert count % 2 == 0 and count <= 2 * self.n
        return ref.at[pl.ds(0, 2), pl.ds(0, count // 2 * rows)]

    def done(self, ref, count, sem):
        part = self.span(ref, count)
        pltpu.make_async_copy(part, part, sem).wait()

    def new(self, ref, layer, k):
        rows = ref.shape[1] // self.n
        return ref.at[layer, pl.ds(pl.multiple_of(self.at(k) * rows, ROWS), rows)]

    def greet(self):
        for way in WAYS:
            pl.semaphore_signal(pltpu.get_barrier_semaphore(), inc=1, device_id={"dp": self.at(way)}, device_id_type=MESH)

    def greeted(self):
        pl.semaphore_wait(pltpu.get_barrier_semaphore(), 2)

    def send(self, source, target, send_sem, recv_sem, way):
        return pltpu.make_async_remote_copy(
            src_ref=source, dst_ref=target, send_sem=send_sem, recv_sem=recv_sem, device_id={"dp": self.at(way)}, device_id_type=MESH
        )


def each(rows, body):
    def step(i, _):
        body(pl.ds(pl.multiple_of(i * ROWS, ROWS), ROWS))
        return 0

    lax.fori_loop(0, rows // ROWS, step, 0)


def kernel(ring, *refs):
    refs = iter(refs)
    take = lambda k: [next(refs) for _ in range(k)]
    g_hbm, w_hbm, m_hbm, v_hbm = take(3), take(3), take(3), take(3)
    w_out, m_out, v_out = take(3), take(3), take(3)
    terms, landed = take(3), take(3)
    load_sem, own_sem, rs_send, rs_recv, ag_send, ag_recv = refs
    n, far, chunks, at, hops, slot = ring.n, ring.far, ring.chunks, ring.at, ring.hops, ring.slot

    def load(c, k, sem):
        a, layer = chunks[c]
        return pltpu.make_async_copy(g_hbm[a].at[layer, at(k)], terms[a].at[layer, at(k)], sem)

    def others(c):
        return [k for k in range(n) if k not in [way * hops(c, way) % n for way in WAYS]]

    def loaded(c):
        a, layer = chunks[c]
        some = pl.ds(0, len(others(c)))
        pltpu.make_async_copy(g_hbm[a].at[layer, some], terms[a].at[layer, some], load_sem.at[c]).wait()

    ring.greet()

    def sum_copy(c, way, s):
        a, layer = chunks[c]
        left = hops(c, way) - s + 1
        source = g_hbm[a].at[layer, at(way * left)] if s == 1 else landed[a].at[layer, slot(c, way, s - 1)]
        return ring.send(source, landed[a].at[layer, slot(c, way, s)], rs_send.at[a], rs_recv.at[c * far + s - 1], way)

    def sums_arrived(c, s):
        a, layer = chunks[c]
        some = landed[a].at[layer, pl.ds(0, sum(s <= hops(c, way) for way in WAYS))]
        pltpu.make_async_copy(some, some, rs_recv.at[c * far + s - 1]).wait()

    def new_copy(c, way, s, k):
        a, layer = chunks[c]
        block = ring.new(w_out[a], layer, k)
        return ring.send(block, block, ag_send.at[2 * c + ring.late(c, s)], ag_recv.at[c * far + s - 1], way)

    def add(c, way, s):
        a, layer = chunks[c]
        sums, mine = landed[a].at[layer, slot(c, way, s)], terms[a].at[layer, at(way * (hops(c, way) - s))]

        def body(rows):
            sums[rows] = (sums[rows].astype(jnp.float32) + mine[rows].astype(jnp.float32)).astype(jnp.bfloat16)

        each(sums.shape[0], body)

    def update(c):
        a, layer = chunks[c]
        one = landed[a].at[layer, slot(c, 1, hops(c, 1))]
        two = landed[a].at[layer, slot(c, -1, hops(c, -1))]
        mine, w, m, v = terms[a].at[layer, at(0)], ring.new(w_out[a], layer, 0), m_out[a].at[layer], v_out[a].at[layer]

        def body(rows):
            g = one[rows].astype(jnp.float32) + two[rows].astype(jnp.float32) + mine[rows].astype(jnp.float32)
            g = g.astype(jnp.bfloat16).astype(jnp.float32)
            w[rows], m[rows], v[rows] = adamw(w[rows].astype(jnp.float32), m[rows], v[rows], g)

        each(one.shape[0], body)

    ring.greeted()
    for c, way in ring.both:
        sum_copy(c, way, 1).start()
    for c, (a, layer) in enumerate(chunks):
        for k in others(c):
            load(c, k, load_sem.at[c]).start()
    for c, (a, layer) in enumerate(chunks):
        pltpu.make_async_copy(w_hbm[a].at[layer, at(0)], ring.new(w_out[a], layer, 0), own_sem.at[0]).start()
    for a in range(3):
        pltpu.make_async_copy(m_hbm[a], m_out[a], own_sem.at[1 + a]).start()
        pltpu.make_async_copy(v_hbm[a], v_out[a], own_sem.at[4 + a]).start()

    for s in range(1, far):
        for c in range(len(chunks)):
            if s == 1:
                loaded(c)
            sums_arrived(c, s)
            for way in WAYS:
                if s < hops(c, way):
                    add(c, way, s)
                    sum_copy(c, way, s + 1).start()
    ring.done(w_out[0], len(chunks), own_sem.at[0])
    for a in range(3):
        pltpu.make_async_copy(m_hbm[a], m_out[a], own_sem.at[1 + a]).wait()
        pltpu.make_async_copy(v_hbm[a], v_out[a], own_sem.at[4 + a]).wait()
    for c in range(len(chunks)):
        sums_arrived(c, far)
        update(c)
        for way in WAYS:
            new_copy(c, way, 1, 0).start()

    def unless_late(late, body):
        if late:
            pl.when(jnp.logical_not(ring.waits()))(body)
        else:
            body()

    for s in range(1, far + 1):
        for c, (a, layer) in enumerate(chunks):
            count = sum(s <= hops(c, way) for way in WAYS)
            unless_late(ring.late(c, s), lambda: ring.done(w_out[a], count, ag_recv.at[c * far + s - 1]))
            for way in WAYS:
                if s < hops(c, way):
                    unless_late(ring.late(c, s + 1), new_copy(c, way, s + 1, -way * s).start)
    for a in range(3):
        pltpu.make_async_copy(landed[a], landed[a], rs_send.at[a]).wait()
    for c, (a, layer) in enumerate(chunks):
        for late in (False, True):
            count = sum(ring.late(c, s) == late for way in WAYS for s in range(1, hops(c, way) + 1))
            unless_late(late, lambda: ring.done(w_out[a], count, ag_send.at[2 * c + late]))


def place(ring, c, way, s):
    a, layer = ring.chunks[c]
    return (a, layer, 0) if s == ring.far else (a, layer, 1 if way == 1 else 2)


def last(ring, *refs):
    w, out = refs[:3], refs[3:6]
    send_sem, recv_sem = refs[6:]
    late = ring.late_hops()
    shared = [(c, way, ring.far) for c, way in ring.both if c == 0]
    first = [hop for hop in late if not ring.late(hop[0], hop[2] - 1) and hop not in shared]
    then = [hop for hop in late if ring.late(hop[0], hop[2] - 1)]
    ring.greet()
    ring.greeted()

    def copy(c, way, s):
        a, layer = ring.chunks[c]
        if ring.late(c, s - 1):
            b, *where = place(ring, c, way, s - 1)
            source = out[b].at[*where]
        else:
            source = ring.new(w[a], layer, -way * (s - 1))
        b, *where = place(ring, c, way, s)
        if (c, way, s) in shared:
            side = source.shape[0] * 3 // 10 // 8 * 8
            rows = pl.ds(0, source.shape[0] - side) if (c, way, s) in late else pl.ds(source.shape[0] - side, side)
            return ring.send(source.at[rows], out[b].at[*where, rows], send_sem.at[0], recv_sem.at[0], way)
        if (c, way, s + 1) in then:
            i = 1 + then.index((c, way, s + 1))
        else:
            i = 0
        return ring.send(source, out[b].at[*where], send_sem.at[0], recv_sem.at[i], way)

    @pl.when(ring.waits())
    def _():
        for hop in sorted(first, key=lambda hop: (hop[2], hop[0])):
            copy(*hop).start()
        for c, way, s in then:
            copy(c, way, s - 1).wait_recv()
            copy(c, way, s).start()
        for hop in shared:
            copy(*hop).start()
        ring.done(w[0], len(late), send_sem.at[0])
        ring.done(w[0], len(late) - len(then), recv_sem.at[0])


def put(ring, *refs):
    here, there, sem = refs[:9], refs[9:18], refs[18]
    late = {(c, -way * s % ring.n) for c, way, s in ring.late_hops()}

    def whole(i):
        return pltpu.make_async_copy(here[i], there[i], sem.at[i])

    for i in range(3, 9):
        whole(i).start()

    @pl.when(jnp.logical_not(ring.waits()))
    def _():
        for i in range(3):
            whole(i).start()
        for i in range(3):
            whole(i).wait()

    @pl.when(ring.waits())
    def _():
        blocks = [(c, k) for c in range(len(ring.chunks)) for k in range(ring.n) if (c, k) not in late]
        for c, k in blocks:
            a, layer = ring.chunks[c]
            pltpu.make_async_copy(ring.new(here[a], layer, k), ring.new(there[a], layer, k), sem.at[9 + c]).start()
        for c, (a, layer) in enumerate(ring.chunks):
            count = sum(c == other for other, _ in blocks)
            pltpu.make_async_copy(ring.span(here[a], count), ring.span(there[a], count), sem.at[9 + c]).wait()

    for i in range(3, 9):
        whole(i).wait()


def put_last(ring, *refs):
    blocks, _, whole, sem = refs[:3], refs[3:6], refs[6:9], refs[9]

    @pl.when(ring.waits())
    def _():
        for c, way, s in ring.late_hops():
            a, layer, which = place(ring, c, way, s)
            pltpu.make_async_copy(blocks[a].at[layer, which], ring.new(whole[a], layer, -way * s), sem.at[0]).start()
        ring.done(whole[0], len(ring.late_hops()), sem.at[0])


def solution(mesh):
    n = mesh.shape["dp"]

    def step(*arrays):
        terms, weights, m, v = (arrays[i : i + 3] for i in (0, 3, 6, 9))
        ring = Ring(n, weights[0].shape[0])
        blocked = lambda w: w.reshape(ring.layers, n, w.shape[-2] // n, w.shape[-1])
        vmem = lambda x: pltpu.VMEM(x.shape, x.dtype)
        hbm = lambda x: pltpu.HBM(x.shape, x.dtype)
        keep = lambda space, arrays: [pltpu.with_memory_space_constraint(x, space) for x in arrays]
        spec = lambda space, k: [pl.BlockSpec(memory_space=space)] * k
        blocks = [blocked(w) for w in weights]
        arrived = [jax.ShapeDtypeStruct((ring.layers, n - 1, *b.shape[2:]), b.dtype) for b in blocks]
        ends = [jax.ShapeDtypeStruct((ring.layers, 3, *b.shape[2:]), b.dtype) for b in blocks]
        assert len({b.size for b in blocks}) == 1

        out = pl.pallas_call(
            lambda *refs: kernel(ring, *refs),
            name="step",
            out_shape=[vmem(x) for x in (*weights, *m, *v)],
            in_specs=spec(pltpu.HBM, 12),
            out_specs=spec(pltpu.VMEM, 9),
            scratch_shapes=[
                *(pltpu.VMEM(x.shape, x.dtype) for x in (*blocks, *arrived)),
                *(pltpu.SemaphoreType.DMA((k,)) for k in (len(ring.chunks), 7)),
                *(pltpu.SemaphoreType.DMA((k,)) for k in (3, len(ring.chunks) * ring.far, 2 * len(ring.chunks), len(ring.chunks) * ring.far)),
            ],
            compiler_params=pltpu.CompilerParams(collective_id=0, has_side_effects=True, vmem_limit_bytes=40 << 20),
        )(*keep(pltpu.HBM, [blocked(t[0]) for t in terms] + blocks + [*m, *v]))
        stored = pl.pallas_call(
            lambda *refs: put(ring, *refs),
            name="put",
            out_shape=[hbm(x) for x in out],
            in_specs=spec(pltpu.VMEM, 9),
            out_specs=spec(pltpu.HBM, 9),
            scratch_shapes=[pltpu.SemaphoreType.DMA((9 + len(ring.chunks),))],
            compiler_params=pltpu.CompilerParams(has_side_effects=True, vmem_limit_bytes=20 << 20),
        )(*keep(pltpu.VMEM, out))
        rest = pl.pallas_call(
            lambda *refs: last(ring, *refs),
            name="last",
            out_shape=[vmem(x) for x in ends],
            in_specs=spec(pltpu.VMEM, 3),
            out_specs=spec(pltpu.VMEM, 3),
            scratch_shapes=[pltpu.SemaphoreType.DMA((1,)), pltpu.SemaphoreType.DMA((LATE + 1,))],
            compiler_params=pltpu.CompilerParams(collective_id=1, has_side_effects=True, vmem_limit_bytes=20 << 20),
        )(*keep(pltpu.VMEM, out[:3]))
        whole = pl.pallas_call(
            lambda *refs: put_last(ring, *refs),
            name="put_last",
            out_shape=[hbm(w) for w in weights],
            in_specs=spec(pltpu.VMEM, 3) + spec(pltpu.HBM, 3),
            out_specs=spec(pltpu.HBM, 3),
            input_output_aliases={3: 0, 4: 1, 5: 2},
            scratch_shapes=[pltpu.SemaphoreType.DMA((1,))],
            compiler_params=pltpu.CompilerParams(has_side_effects=True, vmem_limit_bytes=20 << 20),
        )(*keep(pltpu.VMEM, rest), *keep(pltpu.HBM, stored[:3]))
        return (*whole, *stored[3:])

    all_of, cut = P(None, None, None), P(None, "dp", None)
    return jax.shard_map(
        step,
        mesh=mesh,
        in_specs=(P(("rep", "dp"), None, None, None),) * 3 + (all_of,) * 3 + (cut,) * 6,
        out_specs=(P("rep", None, None),) * 3 + (P("rep", "dp", None),) * 6,
        check_vma=False,
    )
```
